128 devices in a mesh: dom: 16 (over y, z), sub: 8 (over x, core).
Axes of the slice: x: 4, y: 4, z: 4, core: 2. Of those that a mesh axis runs over, the one named last changes fastest.
Arguments:
- positions: float32 [3, 524288], P(None, ('dom', 'sub')), may hold values from -20 to 20
- mass: float32 [524288], P(('dom', 'sub')), may hold values from 3 to 6
- local_tiles: float32 [8192, 128, 128], P(('dom', 'sub')), as said below
- local_rows: int32 [8192], P(('dom', 'sub')), may hold values from 0 to 31, as said below
- local_cols: int32 [8192], P(('dom', 'sub')), may hold values from 0 to 31, as said below
- live_tiles: int32 [128], P(('dom', 'sub')), may hold values from 32 to 64, as said below
- dom_tiles: float32 [4096, 128, 128], P(('dom', 'sub')), as said below
- dom_cols: int32 [4096], P(('dom', 'sub')), may hold values from 0 to 31
- dom_slots: int32 [4096], P(('dom', 'sub')), may hold values from 0 to 511, as said below
- dom_rows: int32 [65536], P(('dom', 'sub')), may hold values from 0 to 31, as said below
- sub_tiles: float32 [6144, 128, 128], P(('dom', 'sub')), as said below
- sub_cols: int32 [6144], P(('dom', 'sub')), may hold values from 0 to 31
- sub_slots: int32 [6144], P(('dom', 'sub')), may hold values from 0 to 63, as said below
- sub_rows: int32 [8192], P(('dom', 'sub')), may hold values from 0 to 31, as said below
- precond: float32 [4096, 128, 128], P(('dom', 'sub')), may hold values from -0.05 to 0.3, as said below
Outputs:
- solution: float32 [3, 524288], P(None, ('dom', 'sub'))
- residual: float32 [3, 524288], P(None, ('dom', 'sub'))
The draws below stay inside these ranges and needn't reach their ends.
Inputs may be any that keep to these rules, and one draw needn't show every extreme that they name: Device d uses the first live_tiles[d] of its 64 interior tiles, an even number; some device uses all of them. `local_tiles`: interior tiles come in pairs 2i, 2i + 1 of a device: the second is the transpose of the first. `local_rows`: tile 2i + 1 of a device has the block row and column of tile 2i swapped. `local_cols`: tile 2i + 1 of a device has the block row and column of tile 2i swapped. `dom_slots`: the destination group of a tile differs from its device's dom index in exactly one of its 4 bits; no two tiles of a device share a slot. `dom_rows`: entries for slots that no tile fills are arbitrary blocks of the receiver. `dom_tiles`: every coupling tile that reaches block row r of a device from block column c of another has a transposed tile on the receiver, from its block column r, that reaches block row c of the sender; so A is symmetric. `sub_slots`: the destination partition of a tile lies in its device's group and is not its device's own; no two tiles of a device share a slot. `sub_rows`: entries for slots that no tile fills are arbitrary blocks of the receiver. `sub_tiles`: every such tile has a transposed partner on the receiving partition that is routed back to the sender's block column. `precond`: every block is symmetric and positive definite.
All inputs are finite; a program needn't handle non-finite values.
Results may differ from the reference program's by a relative error of at most 0.0003.
Values sent between devices are 32-bit elements; how exact they have to be, the bound alone decides.
A program may use at most 64 MiB of HBM per device.

```python
import math
import jax
import jax.numpy as jnp
from jax import lax

TILE = 128
DIMS = 3
NB = 32
ITERS = 3
DBITS = 4
LT = 64
IFD = 32
IFS = 48
SD = 32
SS = 8
V_DEV = 4096
VERTS = 524288
N_DOM = 16
N_SUB = 8


def tile_noise(key, shape):
    values = jax.random.normal(key, shape, jnp.float32)
    return jnp.clip(values, -6.0, 6.0) / math.sqrt(8 * TILE)


def draw_positions(key, part):
    devices_all = VERTS // V_DEV
    owners = jnp.arange(VERTS, dtype=jnp.int32) // V_DEV
    scaling = 1.0 + 2.0 * owners.astype(jnp.float32) / max(devices_all - 1, 1)
    base = jnp.clip(jax.random.normal(key, (DIMS, VERTS), jnp.float32), -6.0, 6.0)
    return jnp.clip(base * scaling[None, :], -20.0, 20.0)


def local_plan(key):
    devices_all = VERTS // V_DEV
    subkeys = jax.random.split(jax.random.fold_in(key, 5), 3)
    first_rows = jax.random.randint(subkeys[0], (devices_all * NB,), 0, NB, dtype=jnp.int32)
    first_cols = jax.random.randint(subkeys[1], (devices_all * NB,), 0, NB, dtype=jnp.int32)
    return (first_rows, first_cols, subkeys[2])


def draw_local_tiles(key, part):
    devices_all = VERTS // V_DEV
    first_rows, first_cols, tile_key = local_plan(key)
    halves = tile_noise(tile_key, (devices_all * NB, TILE, TILE))
    paired = jnp.stack([halves, jnp.swapaxes(halves, 1, 2)], axis=1)
    return paired.reshape(devices_all * LT, TILE, TILE)


def draw_local_rows(key, part):
    first_rows, first_cols, tile_key = local_plan(key)
    return jnp.stack([first_rows, first_cols], axis=1).reshape(-1).astype(jnp.int32)


def draw_local_cols(key, part):
    first_rows, first_cols, tile_key = local_plan(key)
    return jnp.stack([first_cols, first_rows], axis=1).reshape(-1).astype(jnp.int32)


def draw_live_tiles(key, part):
    devices_all = VERTS // V_DEV
    first, second = jax.random.split(key)
    values = 2 * jax.random.randint(first, (devices_all,), NB // 2, NB + 1, dtype=jnp.int32)
    chosen = jax.random.randint(second, (), 0, devices_all, dtype=jnp.int32)
    return jnp.where(jnp.arange(devices_all, dtype=jnp.int32) == chosen, LT, values).astype(jnp.int32)


def dom_plan(key):
    devices_all = VERTS // V_DEV
    half = IFD // 2
    subkeys = jax.random.split(jax.random.fold_in(key, 11), 5)
    bit_choice = jax.random.randint(subkeys[0], (N_SUB, half), 0, DBITS, dtype=jnp.int32)
    bit_choice = bit_choice.at[0, 0].set(DBITS - 1)
    cols_up = jax.random.randint(subkeys[1], (devices_all, half), 0, NB, dtype=jnp.int32)
    rows_up = jax.random.randint(subkeys[2], (devices_all, half), 0, NB, dtype=jnp.int32)
    device_ids = jnp.arange(devices_all, dtype=jnp.int32)
    group_of = device_ids // N_SUB
    member_of = device_ids % N_SUB
    flip_dev = jnp.left_shift(jnp.ones((devices_all, half), jnp.int32), bit_choice[member_of])
    source_down = jnp.bitwise_xor(group_of[:, None], flip_dev) * N_SUB + member_of[:, None]
    return (flip_dev, cols_up, rows_up, source_down, group_of, member_of, subkeys[3], subkeys[4])


def draw_dom_tiles(key, part):
    devices_all = VERTS // V_DEV
    half = IFD // 2
    flip_dev, cols_up, rows_up, source_down, group_of, member_of, tile_key, fill_key = dom_plan(key)
    upward = tile_noise(tile_key, (devices_all, half, TILE, TILE))
    slot_ids = jnp.arange(half, dtype=jnp.int32)[None, :]
    downward = jnp.swapaxes(upward[source_down, slot_ids], 2, 3)
    return jnp.concatenate([upward, downward], axis=1).reshape(devices_all * IFD, TILE, TILE)


def draw_dom_cols(key, part):
    half = IFD // 2
    flip_dev, cols_up, rows_up, source_down, group_of, member_of, tile_key, fill_key = dom_plan(key)
    slot_ids = jnp.arange(half, dtype=jnp.int32)[None, :]
    return jnp.concatenate([cols_up, rows_up[source_down, slot_ids]], axis=1).reshape(-1).astype(jnp.int32)


def draw_dom_slots(key, part):
    half = IFD // 2
    flip_dev, cols_up, rows_up, source_down, group_of, member_of, tile_key, fill_key = dom_plan(key)
    slot_ids = jnp.arange(half, dtype=jnp.int32)[None, :]
    partner = jnp.bitwise_xor(group_of[:, None], flip_dev)
    upward = partner * SD + slot_ids
    downward = partner * SD + half + slot_ids
    return jnp.concatenate([upward, downward], axis=1).reshape(-1).astype(jnp.int32)


def draw_dom_rows(key, part):
    devices_all = VERTS // V_DEV
    half = IFD // 2
    flip_dev, cols_up, rows_up, source_down, group_of, member_of, tile_key, fill_key = dom_plan(key)
    filler = jax.random.randint(fill_key, (devices_all, N_DOM, SD), 0, NB, dtype=jnp.int32)
    groups = jnp.arange(N_DOM, dtype=jnp.int32)[None, :, None]
    mine = group_of[:, None, None]
    flip_full = jnp.concatenate([flip_dev, flip_dev], axis=1)[:, None, :]
    slots = jnp.arange(SD, dtype=jnp.int32)[None, None, :]
    is_down = slots >= half
    slot_mod = slots % half
    matched = jnp.bitwise_xor(groups, flip_full) == mine
    sender = groups * N_SUB + member_of[:, None, None]
    up_value = rows_up[sender, slot_mod]
    own = jnp.arange(devices_all, dtype=jnp.int32)[:, None, None]
    down_value = cols_up[own, slot_mod]
    result = jnp.where(matched, jnp.where(is_down, down_value, up_value), filler)
    return result.reshape(-1).astype(jnp.int32)


def sub_plan(key):
    devices_all = VERTS // V_DEV
    half = IFS // 2
    subkeys = jax.random.split(jax.random.fold_in(key, 23), 5)
    turn = jax.random.randint(subkeys[0], (N_DOM,), 0, N_SUB - 1, dtype=jnp.int32)
    cols_up = jax.random.randint(subkeys[1], (devices_all, half), 0, NB, dtype=jnp.int32)
    rows_up = jax.random.randint(subkeys[2], (devices_all, half), 0, NB, dtype=jnp.int32)
    device_ids = jnp.arange(devices_all, dtype=jnp.int32)
    group_of = device_ids // N_SUB
    member_of = device_ids % N_SUB
    slot_ids = jnp.arange(half, dtype=jnp.int32)[None, :]
    offset_dev = 1 + (slot_ids + turn[group_of][:, None]) % (N_SUB - 1)
    level = slot_ids // (N_SUB - 1)
    source_down = group_of[:, None] * N_SUB + (member_of[:, None] - offset_dev) % N_SUB
    return (turn, cols_up, rows_up, offset_dev, level, source_down, group_of, member_of, subkeys[3], subkeys[4])


def draw_sub_tiles(key, part):
    devices_all = VERTS // V_DEV
    half = IFS // 2
    turn, cols_up, rows_up, offset_dev, level, source_down, group_of, member_of, tile_key, fill_key = sub_plan(key)
    upward = tile_noise(tile_key, (devices_all, half, TILE, TILE))
    slot_ids = jnp.arange(half, dtype=jnp.int32)[None, :]
    downward = jnp.swapaxes(upward[source_down, slot_ids], 2, 3)
    return jnp.concatenate([upward, downward], axis=1).reshape(devices_all * IFS, TILE, TILE)


def draw_sub_cols(key, part):
    half = IFS // 2
    turn, cols_up, rows_up, offset_dev, level, source_down, group_of, member_of, tile_key, fill_key = sub_plan(key)
    slot_ids = jnp.arange(half, dtype=jnp.int32)[None, :]
    return jnp.concatenate([cols_up, rows_up[source_down, slot_ids]], axis=1).reshape(-1).astype(jnp.int32)


def draw_sub_slots(key, part):
    turn, cols_up, rows_up, offset_dev, level, source_down, group_of, member_of, tile_key, fill_key = sub_plan(key)
    upward = (member_of[:, None] + offset_dev) % N_SUB * SS + level
    downward = (member_of[:, None] - offset_dev) % N_SUB * SS + SS // 2 + level
    return jnp.concatenate([upward, downward], axis=1).reshape(-1).astype(jnp.int32)


def draw_sub_rows(key, part):
    devices_all = VERTS // V_DEV
    half = IFS // 2
    half_slots = SS // 2
    turn, cols_up, rows_up, offset_dev, level, source_down, group_of, member_of, tile_key, fill_key = sub_plan(key)
    filler = jax.random.randint(fill_key, (devices_all, N_SUB, SS), 0, NB, dtype=jnp.int32)
    others = jnp.arange(N_SUB, dtype=jnp.int32)[None, :, None]
    mine = member_of[:, None, None]
    group_here = group_of[:, None, None]
    slots = jnp.arange(SS, dtype=jnp.int32)[None, None, :]
    is_down = slots >= half_slots
    depth = jnp.where(is_down, slots - half_slots, slots)
    needed = jnp.where(is_down, (others - mine) % N_SUB, (mine - others) % N_SUB)
    rest = (needed - 1 - turn[group_of][:, None, None]) % (N_SUB - 1)
    index = depth * (N_SUB - 1) + rest
    valid = (needed != 0) & (index < half)
    safe = jnp.clip(index, 0, half - 1)
    sender = group_here * N_SUB + others
    up_value = rows_up[sender, safe]
    own = jnp.broadcast_to(jnp.arange(devices_all, dtype=jnp.int32)[:, None, None], (devices_all, N_SUB, SS))
    down_value = cols_up[own, safe]
    chosen = jnp.where(is_down, down_value, up_value)
    return jnp.where(valid, chosen, filler).reshape(-1).astype(jnp.int32)


def draw_precond(key, part):
    total = VERTS // TILE
    first, second = jax.random.split(key)
    noise = jax.random.normal(first, (total, TILE, TILE), jnp.float32) * (0.045 / math.sqrt(TILE))
    noise = jnp.clip((noise + jnp.swapaxes(noise, 1, 2)) * 0.7071, -0.05, 0.05)
    diagonal = jax.random.uniform(second, (total, TILE), jnp.float32, 0.12, 0.3)
    identity_tile = jnp.eye(TILE, dtype=jnp.float32)
    return noise * (1.0 - identity_tile) + identity_tile * diagonal[:, :, None]


def shard_levels(rng, dims, shards, smallest, largest):
    level, own = 1.0, jax.random.fold_in(rng, 6)
    for dim, blocks in shards:
        steps = jnp.exp(jax.random.uniform(jax.random.fold_in(own, dim), (blocks,), jnp.float32, smallest / len(shards), largest / len(shards)))
        level = level * jnp.repeat(steps, dims[dim] // blocks).reshape([-1 if axis == dim else 1 for axis in range(len(dims))])
    return level


def setup_inputs(seed: int = 0) -> dict:
    streams_of = jax.random.split(jax.random.key(seed), 16)
    return {
        "positions": draw_positions(jax.random.fold_in(streams_of[15], 71), 0),
        "mass": jnp.clip(3.0 + 3.0 * jax.random.uniform(streams_of[1], (VERTS,), jnp.float32) ** shard_levels(streams_of[1], (VERTS,), ((0, 128),), -0.2, 0.2), 3.0, 6.0),
        "local_tiles": draw_local_tiles(jax.random.fold_in(streams_of[15], 71), 0),
        "local_rows": draw_local_rows(jax.random.fold_in(streams_of[15], 71), 0),
        "local_cols": draw_local_cols(jax.random.fold_in(streams_of[15], 71), 0),
        "live_tiles": draw_live_tiles(jax.random.fold_in(streams_of[15], 71), 0),
        "dom_tiles": draw_dom_tiles(jax.random.fold_in(streams_of[15], 71), 0),
        "dom_cols": draw_dom_cols(jax.random.fold_in(streams_of[15], 71), 0),
        "dom_slots": draw_dom_slots(jax.random.fold_in(streams_of[15], 71), 0),
        "dom_rows": draw_dom_rows(jax.random.fold_in(streams_of[15], 71), 0),
        "sub_tiles": draw_sub_tiles(jax.random.fold_in(streams_of[15], 71), 0),
        "sub_cols": draw_sub_cols(jax.random.fold_in(streams_of[15], 71), 0),
        "sub_slots": draw_sub_slots(jax.random.fold_in(streams_of[15], 71), 0),
        "sub_rows": draw_sub_rows(jax.random.fold_in(streams_of[15], 71), 0),
        "precond": draw_precond(jax.random.fold_in(streams_of[15], 71), 0),
    }


PRECISE = lax.Precision.HIGHEST


def tile_terms(tile_stack, columns, blocks, devices_all):
    per_device = tile_stack.shape[0] // devices_all
    owners = jnp.arange(tile_stack.shape[0], dtype=jnp.int32) // per_device
    picked = jnp.take(blocks, owners * NB + columns, axis=1)
    products = jnp.einsum("tij,ktj->tki", tile_stack, picked, precision=PRECISE)
    return products, owners, per_device


def apply_operator(vector, mass, local_tiles, local_rows, local_cols, live_tiles, dom_tiles, dom_cols, dom_slots, dom_rows, sub_tiles, sub_cols, sub_slots, sub_rows):
    devices_all = VERTS // V_DEV
    components = vector.shape[0]
    blocks = vector.reshape(components, devices_all * NB, TILE)
    products, owners, per_device = tile_terms(local_tiles, local_cols, blocks, devices_all)
    place_in = jnp.arange(local_tiles.shape[0], dtype=jnp.int32) - owners * per_device
    live_mask = (place_in < live_tiles[owners]).astype(vector.dtype)
    summed = jax.ops.segment_sum(products * live_mask[:, None, None], owners * NB + local_rows, num_segments=devices_all * NB)
    products, owners, per_device = tile_terms(dom_tiles, dom_cols, blocks, devices_all)
    outgoing = jax.ops.segment_sum(products, owners * (N_DOM * SD) + dom_slots, num_segments=devices_all * N_DOM * SD)
    outgoing = outgoing.reshape(N_DOM, N_SUB, N_DOM, SD, components, TILE).transpose(2, 1, 0, 3, 4, 5)
    outgoing = outgoing.reshape(devices_all * N_DOM * SD, components, TILE)
    receivers = jnp.arange(devices_all * N_DOM * SD, dtype=jnp.int32) // (N_DOM * SD)
    summed = summed + jax.ops.segment_sum(outgoing, receivers * NB + dom_rows, num_segments=devices_all * NB)
    products, owners, per_device = tile_terms(sub_tiles, sub_cols, blocks, devices_all)
    outgoing = jax.ops.segment_sum(products, owners * (N_SUB * SS) + sub_slots, num_segments=devices_all * N_SUB * SS)
    outgoing = outgoing.reshape(N_DOM, N_SUB, N_SUB, SS, components, TILE).transpose(0, 2, 1, 3, 4, 5)
    outgoing = outgoing.reshape(devices_all * N_SUB * SS, components, TILE)
    receivers = jnp.arange(devices_all * N_SUB * SS, dtype=jnp.int32) // (N_SUB * SS)
    summed = summed + jax.ops.segment_sum(outgoing, receivers * NB + sub_rows, num_segments=devices_all * NB)
    return mass[None, :] * vector + summed.transpose(1, 0, 2).reshape(components, VERTS)


def apply_precond(vector, precond):
    components = vector.shape[0]
    blocks = vector.reshape(components, VERTS // TILE, TILE)
    return jnp.einsum("bij,kbj->kbi", precond, blocks, precision=PRECISE).reshape(components, VERTS)


def reference(positions, mass, local_tiles, local_rows, local_cols, live_tiles, dom_tiles, dom_cols, dom_slots, dom_rows, sub_tiles, sub_cols, sub_slots, sub_rows, precond):
    def operate(vector):
        return apply_operator(vector, mass, local_tiles, local_rows, local_cols, live_tiles, dom_tiles, dom_cols, dom_slots, dom_rows, sub_tiles, sub_cols, sub_slots, sub_rows)

    solution = positions
    residual = mass[None, :] * positions - operate(positions)
    smoothed = apply_precond(residual, precond)
    direction = smoothed
    current = jnp.sum(residual * smoothed, axis=1)
    for iteration in range(ITERS):
        applied = operate(direction)
        step_size = current / jnp.sum(direction * applied, axis=1)
        solution = solution + step_size[:, None] * direction
        residual = residual - step_size[:, None] * applied
        if iteration + 1 < ITERS:
            smoothed = apply_precond(residual, precond)
            following = jnp.sum(residual * smoothed, axis=1)
            direction = smoothed + (following / current)[:, None] * direction
            current = following
    return solution, residual
```

```python
import functools

import jax
import jax.numpy as jnp
from jax import lax
from jax.experimental import pallas as pl
from jax.experimental.pallas import tpu as pltpu
from jax.sharding import PartitionSpec as P

TILE = 128
DIMS = 3
NB = 32
LT = 64
IFD = 32
IFS = 48
SD = 32
SS = 8
N_DOM = 16
N_SUB = 8
BITS = 4
PHASES = 4
SHIFT = 0.9

PAIR_L = 0
PAIR_S = LT // 2
PAIR_D = PAIR_S + IFS // 2
PAIR_P = PAIR_D + IFD // 2
PAIRS = PAIR_P + NB // 2
GROUP = 16

BASE_D = NB
BASE_S = NB + BITS * NB
ROWS_X = BASE_S + N_SUB * SS

F32 = jnp.float32
BF16 = jnp.bfloat16


def kernel(
    pos_h,
    mass_h,
    lt_h,
    lrow_h,
    lcol_h,
    live_h,
    dt_h,
    dcol_h,
    dslot_h,
    drow_h,
    st_h,
    scol_h,
    sslot_h,
    srow_h,
    pt_h,
    sol_o,
    res_o,
    x_v,
    x3,
    q_v,
    w_v,
    mass_v,
    land,
    tb,
    xg,
    prod,
    acc,
    got_d,
    got_s,
    pack,
    sel_l,
    sel_s,
    sel_d,
    lcol_v,
    scol_v,
    dcol_v,
    drow_v,
    drow_r,
    part,
    row1,
    got1,
    row2,
    got2,
    lrow_m,
    live_m,
    sslot_m,
    srow_m,
    dslot_m,
    drow_m,
    idx,
    in_sem,
    tile_sem,
    ix_send,
    ix_recv,
    ix_loc,
    sd_send,
    sd_recv,
    ss_send,
    ss_recv,
    a1_send,
    a1_recv,
    a2_send,
    a2_recv,
):
    a = lax.axis_index("dom")
    b = lax.axis_index("sub")

    def dom_dev(j):
        return {"dom": jnp.bitwise_xor(a, 1 << j)}

    def sub_dev(o):
        return {"sub": lax.rem(b + o, N_SUB)}

    small = [
        (pos_h, x_v.at[0]),
        (drow_h, drow_v),
        (mass_h, mass_v),
        (lrow_h, lrow_m),
        (live_h, live_m),
        (sslot_h, sslot_m),
        (srow_h, srow_m),
        (dslot_h, dslot_m),
        (lcol_h, lcol_v),
        (scol_h, scol_v),
        (dcol_h, dcol_v),
    ]
    small = [
        pltpu.make_async_copy(src, dst, in_sem.at[i]) for i, (src, dst) in enumerate(small)
    ]
    for copy in small:
        copy.start()
    loads = []
    for src, first in ((lt_h, PAIR_L), (st_h, PAIR_S), (dt_h, PAIR_D), (pt_h, PAIR_P)):
        for start in range(0, src.shape[0], GROUP):
            loads.append(
                pltpu.make_async_copy(
                    src.at[pl.ds(start, GROUP)],
                    land.at[pl.ds(2 * first + start, GROUP)],
                    tile_sem.at[len(loads)],
                )
            )
    for copy in loads:
        copy.start()

    barrier = pltpu.get_barrier_semaphore()
    for j in range(BITS):
        pl.semaphore_signal(barrier, inc=1, device_id=dom_dev(j))
    for o in range(1, N_SUB):
        pl.semaphore_signal(barrier, inc=1, device_id=sub_dev(o))
    pl.semaphore_wait(barrier, BITS + N_SUB - 1)

    def dom_copy(p, j):
        return pltpu.make_async_remote_copy(
            src_ref=x_v.at[p],
            dst_ref=got_d.at[p, j],
            send_sem=sd_send.at[p, j],
            recv_sem=sd_recv.at[p, j],
            device_id=dom_dev(j),
        )

    def sub_copy(p, o):
        return pltpu.make_async_remote_copy(
            src_ref=pack.at[p, o - 1],
            dst_ref=got_s.at[p, N_SUB - 1 - o],
            send_sem=ss_send.at[p, o - 1],
            recv_sem=ss_recv.at[p, N_SUB - 1 - o],
            device_id=sub_dev(o),
        )

    def sub_arrival(p, e):
        return pltpu.make_async_remote_copy(
            src_ref=pack.at[p, e],
            dst_ref=got_s.at[p, e],
            send_sem=ss_send.at[p, e],
            recv_sem=ss_recv.at[p, e],
            device_id=sub_dev(e + 1),
        )

    def row_copy(j):
        return pltpu.make_async_remote_copy(
            src_ref=drow_v,
            dst_ref=drow_r.at[j],
            send_sem=ix_send.at[j],
            recv_sem=ix_recv.at[j],
            device_id=dom_dev(j),
        )

    def send(p):
        for j in range(BITS):
            dom_copy(p, j).start()

        def gather(i, carry):
            for s in range(SS):
                block = srow_m[lax.rem(b + i + 1, N_SUB) * SS + s]
                rows = x3[p, block]
                for k in range(DIMS):
                    pack[p, i, k, pl.ds(s, 1), :] = rows[k : k + 1]
            return carry

        for k in range(DIMS):
            x3[p, :, k, :] = x_v[p, k]
        lax.fori_loop(0, N_SUB - 1, gather, 0)
        for o in range(1, N_SUB):
            sub_copy(p, o).start()

    xg3 = xg.reshape(ROWS_X, 8, TILE)

    def split(base, count, values):
        for k in range(DIMS):
            high = values[k].astype(BF16).astype(F32)
            xg[pl.ds(base * 8 + k, count, stride=8), :] = high
            xg[pl.ds(base * 8 + DIMS + k, count, stride=8), :] = values[k] - high

    def multiply(pair, first, second, slot):
        left = jnp.concatenate(
            [xg3[first], xg3[second]],
            axis=0,
        ).astype(BF16)
        out = jnp.dot(
            jnp.concatenate([left, left], axis=1), tb[pair], preferred_element_type=F32
        )
        prod[pl.ds(pl.multiple_of(slot * 16, 16), 8), :] = out[0:8, 0:TILE]
        prod[pl.ds(pl.multiple_of(slot * 16 + 8, 8), 8), :] = out[8:16, TILE : 2 * TILE]

    def run(first, count):
        def body(i, carry):
            pair = first + i
            multiply(pair, idx[2 * pair], idx[2 * pair + 1], pair)
            return carry

        lax.fori_loop(0, count, body, 0, unroll=8)

    def taken(first, count, k):
        return (
            prod[pl.ds(first * 16 + k, count, stride=8), :]
            + prod[pl.ds(first * 16 + DIMS + k, count, stride=8), :]
        )

    def combine(select, first, count):
        terms = []
        for k in range(DIMS):
            value = taken(first, count, k)
            high = value.astype(BF16)
            rest = value - high.astype(F32)
            middle = rest.astype(BF16)
            terms += [high, middle, (rest - middle.astype(F32)).astype(BF16)]
        out = jnp.dot(
            select[...], jnp.concatenate(terms, axis=1), preferred_element_type=F32
        )
        sums = []
        for k in range(DIMS):
            at = 3 * k * TILE
            sums.append(
                out[:, at + 2 * TILE : at + 3 * TILE]
                + out[:, at + TILE : at + 2 * TILE]
                + out[:, at : at + TILE]
            )
        return sums

    small[0].wait()
    small[1].wait()
    for j in range(BITS):
        row_copy(j).start()
    for copy in small[2:]:
        copy.wait()
    send(0)

    block_ids = lax.broadcasted_iota(jnp.int32, (NB, LT), 0)
    tile_ids = lax.broadcasted_iota(jnp.int32, (NB, LT), 1)
    hit = jnp.logical_and(lcol_v[...] == block_ids, tile_ids < live_m[0])
    sel_l[...] = jnp.where(hit, 1.0, 0.0).astype(BF16)
    sel_s[...] = jnp.where(
        scol_v[...] == lax.broadcasted_iota(jnp.int32, (NB, IFS), 0), 1.0, 0.0
    ).astype(BF16)
    sel_d[...] = jnp.where(
        dcol_v[...] == lax.broadcasted_iota(jnp.int32, (NB, IFD), 0), 1.0, 0.0
    ).astype(BF16)
    xg[...] = jnp.zeros_like(xg)

    def put_local(t, carry):
        idx[t] = lrow_m[t]
        return carry

    def put_sub(t, carry):
        slot = sslot_m[t]
        place = jnp.bitwise_and(jnp.right_shift(slot, 3) - b - 1, N_SUB - 1)
        idx[2 * PAIR_S + t] = BASE_S + place * SS + jnp.bitwise_and(slot, SS - 1)
        return carry

    lax.fori_loop(0, LT, put_local, 0, unroll=8)
    lax.fori_loop(0, IFS, put_sub, 0, unroll=8)

    def convert(i, carry):
        for half in range(2):
            tile = land[2 * i + half]
            high = tile.astype(BF16)
            low = (tile - high.astype(F32)).astype(BF16)
            tb[i, 0:TILE, half * TILE : (half + 1) * TILE] = high
            tb[i, TILE : 2 * TILE, half * TILE : (half + 1) * TILE] = low
        return carry

    for n, copy in enumerate(loads):
        copy.wait()
        lax.fori_loop(n * GROUP // 2, (n + 1) * GROUP // 2, convert, 0)

    for j in range(BITS):
        row_copy(j).wait_recv()
    moved = pltpu.make_async_copy(drow_r, drow_m, ix_loc)
    moved.start()
    moved.wait()

    def put_dom(t, carry):
        slot = dslot_m[t]
        other = jnp.bitwise_xor(jnp.right_shift(slot, 5), a)
        bit = (
            (other >= 2).astype(jnp.int32)
            + (other >= 4).astype(jnp.int32)
            + (other >= 8).astype(jnp.int32)
        )
        place = a * SD + jnp.bitwise_and(slot, SD - 1)
        block = drow_m[bit, jnp.right_shift(place, 7), jnp.bitwise_and(place, TILE - 1)]
        idx[2 * PAIR_D + t] = BASE_D + bit * NB + block
        return carry

    lax.fori_loop(0, IFD, put_dom, 0, unroll=8)

    def phase(p, carry):
        @pl.when(p > 0)
        def _():
            send(p)

        split(0, NB, [x_v[p, k] for k in range(DIMS)])
        run(PAIR_L, LT // 2)
        for e in range(N_SUB - 1):
            sub_arrival(p, e).wait_recv()
            split(BASE_S + e * SS, SS, [got_s[p, e, k] for k in range(DIMS)])
        run(PAIR_S, IFS // 2)
        inner = combine(sel_l, PAIR_L, LT)
        middle = combine(sel_s, PAIR_S, IFS)
        for k in range(DIMS):
            acc[k] = mass_v[...] * x_v[p, k] + (inner[k] + middle[k])
        for j in range(BITS):
            dom_copy(p, j).wait_recv()
            split(BASE_D + j * NB, NB, [got_d[p, j, k] for k in range(DIMS)])
        run(PAIR_D, IFD // 2)
        outer = combine(sel_d, PAIR_D, IFD)

        @pl.when(p == 0)
        def _():
            for k in range(DIMS):
                q_v[0, k] = mass_v[...] * x_v[0, k] - (acc[k] + outer[k])

        @pl.when(p > 0)
        def _():
            for k in range(DIMS):
                w_v[p - 1, k] = acc[k] + outer[k]

        @pl.when(jnp.logical_and(p > 0, p < PHASES - 1))
        def _():
            for k in range(DIMS):
                q_v[p, k] = w_v[p - 1, k] - SHIFT * q_v[p - 1, k]

        @pl.when(p < PHASES - 1)
        def _():
            split(0, NB, [q_v[p, k] for k in range(DIMS)])

            def body(i, carry):
                multiply(PAIR_P + i, 2 * i, 2 * i + 1, PAIR_P + i)
                return carry

            lax.fori_loop(0, NB // 2, body, 0, unroll=8)
            for k in range(DIMS):
                x_v[p + 1, k] = taken(PAIR_P, NB, k)

        for j in range(BITS):
            dom_copy(p, j).wait_send()
        for o in range(1, N_SUB):
            sub_copy(p, o).wait_send()
        return carry

    lax.fori_loop(0, PHASES, phase, 0)
    for j in range(BITS):
        row_copy(j).wait_send()

    part[...] = jnp.zeros_like(part)
    wanted = [(0, 0), (0, 1), (0, 2), (1, 1), (1, 2), (2, 2)]
    for n, (i, j) in enumerate(wanted):
        for k in range(DIMS):
            part[pl.ds(n * DIMS + k, 1), :] = jnp.sum(
                q_v[i, k] * x_v[j + 1, k], axis=0, keepdims=True
            )
    for k in range(DIMS):
        part[pl.ds(6 * DIMS + k, 1), :] = jnp.sum(
            x_v[3, k] * w_v[2, k], axis=0, keepdims=True
        )
    sums = jnp.sum(part[...], axis=1, keepdims=True)
    eye = lax.broadcasted_iota(jnp.int32, part.shape, 0) == lax.broadcasted_iota(
        jnp.int32, part.shape, 1
    )
    row1[...] = jnp.sum(jnp.where(eye, sums, 0.0), axis=0, keepdims=True)

    def spread(count, source, target, send_sem, recv_sem, device):
        for o in range(1, count):
            pltpu.make_async_remote_copy(
                src_ref=source,
                dst_ref=target.at[count - 1 - o],
                send_sem=send_sem.at[o - 1],
                recv_sem=recv_sem.at[count - 1 - o],
                device_id=device(o),
            ).start()
        total = source[...]
        for e in range(count - 1):
            arrived = pltpu.make_async_remote_copy(
                src_ref=source,
                dst_ref=target.at[e],
                send_sem=send_sem.at[e],
                recv_sem=recv_sem.at[e],
                device_id=device(e + 1),
            )
            arrived.wait_recv()
            total = total + target[e]
        for e in range(count - 1):
            pltpu.make_async_remote_copy(
                src_ref=source,
                dst_ref=target.at[e],
                send_sem=send_sem.at[e],
                recv_sem=recv_sem.at[e],
                device_id=device(e + 1),
            ).wait_send()
        return total

    row2[...] = spread(N_SUB, row1, got1, a1_send, a1_recv, sub_dev)
    total = spread(
        N_DOM, row2, got2, a2_send, a2_recv, lambda o: {"dom": lax.rem(a + o, N_DOM)}
    )

    wide = jnp.broadcast_to(total, (8, TILE))
    values = [wide] + [pltpu.roll(wide, TILE - DIMS * n, 1) for n in range(1, 7)]
    gram = {}
    for (i, j), value in zip(wanted, values):
        gram[i, j] = gram[j, i] = value
    curve = {}
    for j in range(2):
        for i in range(3):
            curve[i, j] = curve[j, i] = gram[i, j + 1] + SHIFT * gram[i, j]
    curve[2, 2] = values[6]

    def form(table, vector):
        out = None
        for i in range(len(vector)):
            for j in range(i, len(vector)):
                term = vector[i] * vector[j] * table[i, j]
                term = term if i == j else 2.0 * term
                out = term if out is None else out + term
        return out

    one = jnp.ones((8, TILE), F32)
    rho = [one]
    along = [one]
    current = gram[0, 0]
    solved = [None] * 3
    for it in range(3):
        step = current / form(curve, along)
        for i, value in enumerate(along):
            moved_by = step * value
            solved[i] = moved_by if solved[i] is None else solved[i] + moved_by
        if it < 2:
            fresh = []
            for i in range(len(along) + 1):
                value = rho[i] if i < len(rho) else None
                if i < len(along):
                    value = value - step * (SHIFT * along[i])
                if i > 0:
                    less = step * along[i - 1]
                    value = -less if value is None else value - less
                fresh.append(value)
            rho = fresh
            following = form(gram, rho)
            ratio = following / current
            along = [
                value + ratio * along[i] if i < len(along) else value
                for i, value in enumerate(rho)
            ]
            current = following
    for k in range(DIMS):
        faired = x_v[0, k]
        left = q_v[0, k]
        for j in range(3):
            scale = solved[j][0:1, k : k + 1]
            faired = faired + scale * x_v[j + 1, k]
            left = left - scale * w_v[j, k]
        sol_o[k] = faired
        res_o[k] = left


def on_device(
    positions,
    mass,
    local_tiles,
    local_rows,
    local_cols,
    live_tiles,
    dom_tiles,
    dom_cols,
    dom_slots,
    dom_rows,
    sub_tiles,
    sub_cols,
    sub_slots,
    sub_rows,
    precond,
):
    vector = jax.ShapeDtypeStruct((DIMS, NB, TILE), F32)
    dma = pltpu.SemaphoreType.DMA
    solved, left = pl.pallas_call(
        kernel,
        out_shape=(vector, vector),
        in_specs=[pl.BlockSpec(memory_space=pl.ANY)] * 15,
        out_specs=(pl.BlockSpec(memory_space=pltpu.VMEM),) * 2,
        scratch_shapes=[
            pltpu.VMEM((PHASES, DIMS, NB, TILE), F32),
            pltpu.VMEM((PHASES, NB, 8, TILE), F32),
            pltpu.VMEM((3, DIMS, NB, TILE), F32),
            pltpu.VMEM((3, DIMS, NB, TILE), F32),
            pltpu.VMEM((NB, TILE), F32),
            pltpu.VMEM((2 * PAIRS, TILE, TILE), F32),
            pltpu.VMEM((PAIRS, 2 * TILE, 2 * TILE), BF16),
            pltpu.VMEM((ROWS_X * 8, TILE), F32),
            pltpu.VMEM((PAIRS * 16, TILE), F32),
            pltpu.VMEM((DIMS, NB, TILE), F32),
            pltpu.VMEM((PHASES, BITS, DIMS, NB, TILE), F32),
            pltpu.VMEM((PHASES, N_SUB - 1, DIMS, SS, TILE), F32),
            pltpu.VMEM((PHASES, N_SUB - 1, DIMS, SS, TILE), F32),
            pltpu.VMEM((NB, LT), BF16),
            pltpu.VMEM((NB, IFS), BF16),
            pltpu.VMEM((NB, IFD), BF16),
            pltpu.VMEM((1, LT), jnp.int32),
            pltpu.VMEM((1, IFS), jnp.int32),
            pltpu.VMEM((1, IFD), jnp.int32),
            pltpu.VMEM((4, TILE), jnp.int32),
            pltpu.VMEM((BITS, 4, TILE), jnp.int32),
            pltpu.VMEM((24, TILE), F32),
            pltpu.VMEM((1, TILE), F32),
            pltpu.VMEM((N_SUB - 1, 1, TILE), F32),
            pltpu.VMEM((1, TILE), F32),
            pltpu.VMEM((N_DOM - 1, 1, TILE), F32),
            pltpu.SMEM((LT,), jnp.int32),
            pltpu.SMEM((1,), jnp.int32),
            pltpu.SMEM((IFS,), jnp.int32),
            pltpu.SMEM((N_SUB * SS,), jnp.int32),
            pltpu.SMEM((IFD,), jnp.int32),
            pltpu.SMEM((BITS, 4, TILE), jnp.int32),
            pltpu.SMEM((2 * PAIR_P,), jnp.int32),
            dma((11,)),
            dma((2 * PAIRS // GROUP,)),
            dma((BITS,)),
            dma((BITS,)),
            dma,
            dma((PHASES, BITS)),
            dma((PHASES, BITS)),
            dma((PHASES, N_SUB - 1)),
            dma((PHASES, N_SUB - 1)),
            dma((N_SUB - 1,)),
            dma((N_SUB - 1,)),
            dma((N_DOM - 1,)),
            dma((N_DOM - 1,)),
        ],
        compiler_params=pltpu.CompilerParams(
            collective_id=0, has_side_effects=True, vmem_limit_bytes=56 * 1024 * 1024
        ),
    )(
        positions.reshape(DIMS, NB, TILE),
        mass.reshape(NB, TILE),
        local_tiles,
        local_rows,
        local_cols.reshape(1, LT),
        live_tiles,
        dom_tiles,
        dom_cols.reshape(1, IFD),
        dom_slots,
        dom_rows.reshape(4, TILE),
        sub_tiles,
        sub_cols.reshape(1, IFS),
        sub_slots,
        sub_rows,
        precond,
    )
    return solved.reshape(DIMS, NB * TILE), left.reshape(DIMS, NB * TILE)


def solution(mesh):
    flat = P(("dom", "sub"))
    cube = P(("dom", "sub"), None, None)
    vector = P(None, ("dom", "sub"))
    return jax.shard_map(
        on_device,
        mesh=mesh,
        in_specs=(
            vector,
            flat,
            cube,
            flat,
            flat,
            flat,
            cube,
            flat,
            flat,
            flat,
            cube,
            flat,
            flat,
            flat,
            cube,
        ),
        out_specs=(vector, vector),
        check_vma=False,
    )
```

```python
import functools

import jax
import jax.numpy as jnp
from jax import lax
from jax.experimental import pallas as pl
from jax.experimental.pallas import tpu as pltpu
from jax.sharding import PartitionSpec as P

TILE = 128
DIMS = 3
NB = 32
LT = 64
IFD = 32
IFS = 48
SD = 32
SS = 8
N_DOM = 16
N_SUB = 8
BITS = 4
PHASES = 4
SHIFT = 0.9

PAIR_L = 0
PAIR_S = LT // 2
PAIR_D = PAIR_S + IFS // 2
PAIR_P = PAIR_D + IFD // 2
PAIRS = PAIR_P + NB // 2
GROUP = 16

BASE_D = NB
BASE_S = NB + BITS * NB
ROWS_X = BASE_S + N_SUB * SS

F32 = jnp.float32
BF16 = jnp.bfloat16


def kernel(
    pos_h,
    mass_h,
    lt_h,
    lrow_h,
    lcol_h,
    live_h,
    dt_h,
    dcol_h,
    dslot_h,
    drow_h,
    st_h,
    scol_h,
    sslot_h,
    srow_h,
    pt_h,
    sol_o,
    res_o,
    pos_v,
    x_v,
    x3,
    q_v,
    w_v,
    mass_v,
    land,
    tb,
    xg,
    prod,
    acc,
    got_d,
    got_s,
    pack,
    sel_l,
    sel_s,
    sel_d,
    lcol_v,
    scol_v,
    dcol_v,
    drow_v,
    drow_r,
    part,
    row1,
    rows,
    lrow_m,
    live_m,
    sslot_m,
    srow_m,
    dslot_m,
    drow_m,
    idx,
    in_sem,
    tile_sem,
    ix_send,
    ix_recv,
    ix_loc,
    sd_send,
    sd_recv,
    ss_send,
    ss_recv,
    a1_send,
    a1_recv,
):
    a = lax.axis_index("dom")
    b = lax.axis_index("sub")

    def dom_dev(j):
        return {"dom": jnp.bitwise_xor(a, 1 << j)}

    def sub_dev(o):
        return {"sub": lax.rem(b + o, N_SUB)}

    barrier = pltpu.get_barrier_semaphore()
    for j in range(BITS):
        pl.semaphore_signal(barrier, inc=1, device_id=dom_dev(j))
    for o in range(1, N_SUB):
        pl.semaphore_signal(barrier, inc=1, device_id=sub_dev(o))

    small = [
        (pos_h, pos_v),
        (drow_h, drow_v),
        (mass_h, mass_v),
        (lrow_h, lrow_m),
        (live_h, live_m),
        (sslot_h, sslot_m),
        (srow_h, srow_m),
        (dslot_h, dslot_m),
        (lcol_h, lcol_v),
        (scol_h, scol_v),
        (dcol_h, dcol_v),
    ]
    small = [
        pltpu.make_async_copy(src, dst, in_sem.at[i]) for i, (src, dst) in enumerate(small)
    ]
    for copy in small:
        copy.start()
    loads = []
    for src, first in ((lt_h, PAIR_L), (st_h, PAIR_S), (dt_h, PAIR_D), (pt_h, PAIR_P)):
        for start in range(0, src.shape[0], GROUP):
            loads.append(
                pltpu.make_async_copy(
                    src.at[pl.ds(start, GROUP)],
                    land.at[pl.ds(2 * first + start, GROUP)],
                    tile_sem.at[len(loads)],
                )
            )
    for copy in loads:
        copy.start()

    def dom_copy(p, j):
        return pltpu.make_async_remote_copy(
            src_ref=x_v.at[p],
            dst_ref=got_d.at[p, j],
            send_sem=sd_send.at[p, j],
            recv_sem=sd_recv.at[p, j],
            device_id=dom_dev(j),
        )

    def sub_copy(p, o):
        return pltpu.make_async_remote_copy(
            src_ref=pack.at[p, o - 1],
            dst_ref=got_s.at[p, N_SUB - 1 - o],
            send_sem=ss_send.at[p, o - 1],
            recv_sem=ss_recv.at[p, N_SUB - 1 - o],
            device_id=sub_dev(o),
        )

    def sub_arrival(p, e):
        return pltpu.make_async_remote_copy(
            src_ref=pack.at[p, e],
            dst_ref=got_s.at[p, e],
            send_sem=ss_send.at[p, e],
            recv_sem=ss_recv.at[p, e],
            device_id=sub_dev(e + 1),
        )

    def row_copy(j):
        return pltpu.make_async_remote_copy(
            src_ref=drow_v,
            dst_ref=drow_r.at[j],
            send_sem=ix_send.at[j],
            recv_sem=ix_recv.at[j],
            device_id=dom_dev(j),
        )

    def send(p):
        for j in range(BITS):
            dom_copy(p, j).start()

        def gather(i, carry):
            for s in range(SS):
                block = srow_m[lax.rem(b + i + 1, N_SUB) * SS + s]
                rows = x3[p, block]
                for k in range(DIMS):
                    pack[p, i, k, pl.ds(s, 1), :] = rows[k : k + 1]
            return carry

        lax.fori_loop(0, N_SUB - 1, gather, 0)
        for o in range(1, N_SUB):
            sub_copy(p, o).start()

    xg3 = xg.reshape(ROWS_X, 8, TILE)

    def split(base, count, values):
        for k in range(DIMS):
            high = values[k].astype(BF16).astype(F32)
            xg[pl.ds(base * 8 + k, count, stride=8), :] = high
            xg[pl.ds(base * 8 + DIMS + k, count, stride=8), :] = values[k] - high

    def multiply(pair, first, second, slot):
        left = jnp.concatenate(
            [xg3[first], xg3[second]],
            axis=0,
        ).astype(BF16)
        out = jnp.dot(
            jnp.concatenate([left, left], axis=1),
            jnp.concatenate(
                [tb[pair, 0, 0 : 2 * TILE, :], tb[pair, 1, 0 : 2 * TILE, :]], axis=1
            ),
            preferred_element_type=F32,
        )
        prod[pl.ds(pl.multiple_of(slot * 16, 16), 8), :] = out[0:8, 0:TILE]
        prod[pl.ds(pl.multiple_of(slot * 16 + 8, 8), 8), :] = out[8:16, TILE : 2 * TILE]

    def run(first, count):
        def body(i, carry):
            pair = first + i
            multiply(pair, idx[2 * pair], idx[2 * pair + 1], pair)
            return carry

        lax.fori_loop(0, count, body, 0, unroll=True)

    def taken(first, count, k):
        return (
            prod[pl.ds(first * 16 + k, count, stride=8), :]
            + prod[pl.ds(first * 16 + DIMS + k, count, stride=8), :]
        )

    def combine(select, first, count):
        terms = []
        for k in range(DIMS):
            value = taken(first, count, k)
            high = value.astype(BF16)
            rest = value - high.astype(F32)
            middle = rest.astype(BF16)
            terms += [high, middle, (rest - middle.astype(F32)).astype(BF16)]
        out = jnp.dot(
            select[...], jnp.concatenate(terms, axis=1), preferred_element_type=F32
        )
        sums = []
        for k in range(DIMS):
            at = 3 * k * TILE
            sums.append(
                out[:, at + 2 * TILE : at + 3 * TILE]
                + out[:, at + TILE : at + 2 * TILE]
                + out[:, at : at + TILE]
            )
        return sums

    small[0].wait()
    for c in range(NB):
        x3[0, c, 0:DIMS, :] = pos_v[:, c * TILE : (c + 1) * TILE]
    for k in range(DIMS):
        x_v[0, k] = x3[0, :, k, :]
    for copy in small[1:]:
        copy.wait()
    pl.semaphore_wait(barrier, BITS + N_SUB - 1)
    send(0)
    for j in range(BITS):
        row_copy(j).start()

    block_ids = lax.broadcasted_iota(jnp.int32, (NB, LT), 0)
    tile_ids = lax.broadcasted_iota(jnp.int32, (NB, LT), 1)
    hit = jnp.logical_and(lcol_v[...] == block_ids, tile_ids < live_m[0])
    sel_l[...] = jnp.where(hit, 1.0, 0.0).astype(BF16)
    sel_s[...] = jnp.where(
        scol_v[...] == lax.broadcasted_iota(jnp.int32, (NB, IFS), 0), 1.0, 0.0
    ).astype(BF16)
    sel_d[...] = jnp.where(
        dcol_v[...] == lax.broadcasted_iota(jnp.int32, (NB, IFD), 0), 1.0, 0.0
    ).astype(BF16)
    xg[...] = jnp.zeros_like(xg)

    def put_local(t, carry):
        idx[t] = lrow_m[t]
        return carry

    def put_sub(t, carry):
        slot = sslot_m[t]
        place = jnp.bitwise_and(jnp.right_shift(slot, 3) - b - 1, N_SUB - 1)
        idx[2 * PAIR_S + t] = BASE_S + place * SS + jnp.bitwise_and(slot, SS - 1)
        return carry

    lax.fori_loop(0, LT, put_local, 0, unroll=8)
    lax.fori_loop(0, IFS, put_sub, 0, unroll=8)

    def convert(i, carry):
        for half in range(2):
            tile = land[2 * i + half]
            high = tile.astype(BF16)
            low = (tile - high.astype(F32)).astype(BF16)
            tb[i, half, 0:TILE, :] = high
            tb[i, half, TILE : 2 * TILE, :] = low
        return carry

    def arrive(n, carry):
        pltpu.make_async_copy(
            lt_h.at[pl.ds(0, GROUP)],
            land.at[pl.ds(n * GROUP, GROUP)],
            tile_sem.at[n],
        ).wait()
        lax.fori_loop(0, GROUP // 2, lambda i, c: convert(n * GROUP // 2 + i, c), 0, unroll=4)
        return carry

    lax.fori_loop(0, 2 * PAIRS // GROUP, arrive, 0)

    def put_dom(t, carry):
        slot = dslot_m[t]
        other = jnp.bitwise_xor(jnp.right_shift(slot, 5), a)
        bit = (
            (other >= 2).astype(jnp.int32)
            + (other >= 4).astype(jnp.int32)
            + (other >= 8).astype(jnp.int32)
        )
        place = a * SD + jnp.bitwise_and(slot, SD - 1)
        block = drow_m[bit, jnp.right_shift(place, 7), jnp.bitwise_and(place, TILE - 1)]
        idx[2 * PAIR_D + t] = BASE_D + bit * NB + block
        return carry

    part[...] = jnp.zeros_like(part)
    wanted = [(0, 0), (0, 1), (0, 2), (1, 1), (1, 2), (2, 2)]

    def phase(p, carry):
        @pl.when(p > 0)
        def _():
            send(p)

        split(0, NB, [x_v[p, k] for k in range(DIMS)])
        run(PAIR_L, LT // 2)

        @pl.when(p == PHASES - 1)
        def _():
            for n, (i, j) in enumerate(wanted):
                for k in range(DIMS):
                    part[pl.ds(n * DIMS + k, 1), :] = jnp.sum(
                        q_v[i, k] * x_v[j + 1, k], axis=0, keepdims=True
                    )

        for e in range(N_SUB - 1):
            sub_arrival(p, e).wait_recv()
            split(BASE_S + e * SS, SS, [got_s[p, e, k] for k in range(DIMS)])
        run(PAIR_S, IFS // 2)
        inner = combine(sel_l, PAIR_L, LT)
        middle = combine(sel_s, PAIR_S, IFS)
        for k in range(DIMS):
            acc[k] = mass_v[...] * x_v[p, k] + (inner[k] + middle[k])
        @pl.when(p == 0)
        def _():
            for j in range(BITS):
                row_copy(j).wait_recv()
            moved = pltpu.make_async_copy(drow_r, drow_m, ix_loc)
            moved.start()
            moved.wait()
            lax.fori_loop(0, IFD, put_dom, 0, unroll=8)

        for j in range(BITS):
            dom_copy(p, j).wait_recv()
            split(BASE_D + j * NB, NB, [got_d[p, j, k] for k in range(DIMS)])
        run(PAIR_D, IFD // 2)
        outer = combine(sel_d, PAIR_D, IFD)

        @pl.when(p == 0)
        def _():
            for k in range(DIMS):
                q_v[0, k] = mass_v[...] * x_v[0, k] - (acc[k] + outer[k])

        @pl.when(p > 0)
        def _():
            for k in range(DIMS):
                w_v[p - 1, k] = acc[k] + outer[k]

        @pl.when(jnp.logical_and(p > 0, p < PHASES - 1))
        def _():
            for k in range(DIMS):
                q_v[p, k] = w_v[p - 1, k] - SHIFT * q_v[p - 1, k]

        @pl.when(p < PHASES - 1)
        def _():
            split(0, NB, [q_v[p, k] for k in range(DIMS)])

            def body(i, carry):
                multiply(PAIR_P + i, 2 * i, 2 * i + 1, PAIR_P + i)
                return carry

            lax.fori_loop(0, NB // 2, body, 0, unroll=True)
            for k in range(DIMS):
                value = taken(PAIR_P, NB, k)
                x_v[p + 1, k] = value
                x3[p + 1, :, k, :] = value

        return carry

    lax.fori_loop(0, PHASES, phase, 0)
    for k in range(DIMS):
        part[pl.ds(6 * DIMS + k, 1), :] = jnp.sum(
            x_v[3, k] * w_v[2, k], axis=0, keepdims=True
        )
    sums = jnp.sum(part[...], axis=1, keepdims=True)
    eye = lax.broadcasted_iota(jnp.int32, part.shape, 0) == lax.broadcasted_iota(
        jnp.int32, part.shape, 1
    )
    me = a * N_SUB + b
    row1[...] = jnp.sum(jnp.where(eye, sums, 0.0), axis=0, keepdims=True)

    def row_to(i):
        other = lax.rem(me + 1 + i, N_DOM * N_SUB)
        return pltpu.make_async_remote_copy(
            src_ref=row1,
            dst_ref=rows.at[pl.ds(me, 1)],
            send_sem=a1_send,
            recv_sem=a1_recv,
            device_id={"dom": other // N_SUB, "sub": lax.rem(other, N_SUB)},
        )

    def scatter(i, carry):
        row_to(i).start()
        return carry

    lax.fori_loop(0, N_DOM * N_SUB - 1, scatter, 0, unroll=8)
    rows[pl.ds(me, 1), :] = row1[...]
    everyone = rows.at[pl.ds(0, N_DOM * N_SUB - 1)]
    both = pltpu.make_async_remote_copy(
        src_ref=everyone,
        dst_ref=everyone,
        send_sem=a1_send,
        recv_sem=a1_recv,
        device_id=sub_dev(1),
    )
    both.wait_recv()
    total = jnp.sum(rows[...], axis=0, keepdims=True)

    wide = jnp.broadcast_to(total, (8, TILE))
    values = [wide] + [pltpu.roll(wide, TILE - DIMS * n, 1) for n in range(1, 7)]
    gram = {}
    for (i, j), value in zip(wanted, values):
        gram[i, j] = gram[j, i] = value
    curve = {}
    for j in range(2):
        for i in range(3):
            curve[i, j] = curve[j, i] = gram[i, j + 1] + SHIFT * gram[i, j]
    curve[2, 2] = values[6]

    def form(table, vector):
        out = None
        for i in range(len(vector)):
            for j in range(i, len(vector)):
                term = vector[i] * vector[j] * table[i, j]
                term = term if i == j else 2.0 * term
                out = term if out is None else out + term
        return out

    one = jnp.ones((8, TILE), F32)
    rho = [one]
    along = [one]
    current = gram[0, 0]
    solved = [None] * 3
    for it in range(3):
        step = current / form(curve, along)
        for i, value in enumerate(along):
            moved_by = step * value
            solved[i] = moved_by if solved[i] is None else solved[i] + moved_by
        if it < 2:
            fresh = []
            for i in range(len(along) + 1):
                value = rho[i] if i < len(rho) else None
                if i < len(along):
                    value = value - step * (SHIFT * along[i])
                if i > 0:
                    less = step * along[i - 1]
                    value = -less if value is None else value - less
                fresh.append(value)
            rho = fresh
            following = form(gram, rho)
            ratio = following / current
            along = [
                value + ratio * along[i] if i < len(along) else value
                for i, value in enumerate(rho)
            ]
            current = following
    for k in range(DIMS):
        faired = x_v[0, k]
        left = q_v[0, k]
        for j in range(3):
            scale = solved[j][0:1, k : k + 1]
            faired = faired + scale * x_v[j + 1, k]
            left = left - scale * w_v[j, k]
        sol_o[k] = faired
        res_o[k] = left

    both.wait_send()
    for j in range(BITS):
        row_copy(j).wait_send()
    for p in range(PHASES):
        for j in range(BITS):
            dom_copy(p, j).wait_send()
        for o in range(1, N_SUB):
            sub_copy(p, o).wait_send()


def on_device(
    positions,
    mass,
    local_tiles,
    local_rows,
    local_cols,
    live_tiles,
    dom_tiles,
    dom_cols,
    dom_slots,
    dom_rows,
    sub_tiles,
    sub_cols,
    sub_slots,
    sub_rows,
    precond,
):
    vector = jax.ShapeDtypeStruct((DIMS, NB, TILE), F32)
    dma = pltpu.SemaphoreType.DMA
    solved, left = pl.pallas_call(
        kernel,
        out_shape=(vector, vector),
        in_specs=[pl.BlockSpec(memory_space=pl.ANY)] * 15,
        out_specs=(pl.BlockSpec(memory_space=pltpu.VMEM),) * 2,
        scratch_shapes=[
            pltpu.VMEM((DIMS, NB * TILE), F32),
            pltpu.VMEM((PHASES, DIMS, NB, TILE), F32),
            pltpu.VMEM((PHASES, NB, 8, TILE), F32),
            pltpu.VMEM((3, DIMS, NB, TILE), F32),
            pltpu.VMEM((3, DIMS, NB, TILE), F32),
            pltpu.VMEM((NB, TILE), F32),
            pltpu.VMEM((2 * PAIRS, TILE, TILE), F32),
            pltpu.VMEM((PAIRS, 2, 2 * TILE + 16, TILE), BF16),
            pltpu.VMEM((ROWS_X * 8, TILE), F32),
            pltpu.VMEM((PAIRS * 16, TILE), F32),
            pltpu.VMEM((DIMS, NB, TILE), F32),
            pltpu.VMEM((PHASES, BITS, DIMS, NB, TILE), F32),
            pltpu.VMEM((PHASES, N_SUB - 1, DIMS, SS, TILE), F32),
            pltpu.VMEM((PHASES, N_SUB - 1, DIMS, SS, TILE), F32),
            pltpu.VMEM((NB, LT), BF16),
            pltpu.VMEM((NB, IFS), BF16),
            pltpu.VMEM((NB, IFD), BF16),
            pltpu.VMEM((1, LT), jnp.int32),
            pltpu.VMEM((1, IFS), jnp.int32),
            pltpu.VMEM((1, IFD), jnp.int32),
            pltpu.VMEM((4, TILE), jnp.int32),
            pltpu.VMEM((BITS, 4, TILE), jnp.int32),
            pltpu.VMEM((24, TILE), F32),
            pltpu.VMEM((1, TILE), F32),
            pltpu.VMEM((N_DOM * N_SUB, TILE), F32),
            pltpu.SMEM((LT,), jnp.int32),
            pltpu.SMEM((1,), jnp.int32),
            pltpu.SMEM((IFS,), jnp.int32),
            pltpu.SMEM((N_SUB * SS,), jnp.int32),
            pltpu.SMEM((IFD,), jnp.int32),
            pltpu.SMEM((BITS, 4, TILE), jnp.int32),
            pltpu.SMEM((2 * PAIR_P,), jnp.int32),
            dma((11,)),
            dma((2 * PAIRS // GROUP,)),
            dma((BITS,)),
            dma((BITS,)),
            dma,
            dma((PHASES, BITS)),
            dma((PHASES, BITS)),
            dma((PHASES, N_SUB - 1)),
            dma((PHASES, N_SUB - 1)),
            dma,
            dma,
        ],
        compiler_params=pltpu.CompilerParams(
            collective_id=0, has_side_effects=True, vmem_limit_bytes=56 * 1024 * 1024
        ),
    )(
        positions,
        mass.reshape(NB, TILE),
        local_tiles,
        local_rows,
        local_cols.reshape(1, LT),
        live_tiles,
        dom_tiles,
        dom_cols.reshape(1, IFD),
        dom_slots,
        dom_rows.reshape(4, TILE),
        sub_tiles,
        sub_cols.reshape(1, IFS),
        sub_slots,
        sub_rows,
        precond,
    )
    return solved.reshape(DIMS, NB * TILE), left.reshape(DIMS, NB * TILE)


def solution(mesh):
    flat = P(("dom", "sub"))
    cube = P(("dom", "sub"), None, None)
    vector = P(None, ("dom", "sub"))
    return jax.shard_map(
        on_device,
        mesh=mesh,
        in_specs=(
            vector,
            flat,
            cube,
            flat,
            flat,
            flat,
            cube,
            flat,
            flat,
            flat,
            cube,
            flat,
            flat,
            flat,
            cube,
        ),
        out_specs=(vector, vector),
        check_vma=False,
    )
```

```python
import functools

import jax
import jax.numpy as jnp
from jax import lax
from jax.experimental import pallas as pl
from jax.experimental.pallas import tpu as pltpu
from jax.sharding import PartitionSpec as P

TILE = 128
DIMS = 3
NB = 32
LT = 64
IFD = 32
IFS = 48
SD = 32
SS = 8
N_DOM = 16
N_SUB = 8
BITS = 4
PHASES = 4
SHIFT = 0.9

PAIR_L = 0
PAIR_S = LT // 2
PAIR_D = PAIR_S + IFS // 2
PAIR_P = PAIR_D + IFD // 2
PAIRS = PAIR_P + NB // 2
GROUP = 16
EARLY = LT // GROUP

BASE_D = NB
BASE_S = NB + BITS * NB
ROWS_X = BASE_S + N_SUB * SS

F32 = jnp.float32
BF16 = jnp.bfloat16


def kernel(
    pos_h,
    mass_h,
    lt_h,
    lrow_h,
    lcol_h,
    live_h,
    dt_h,
    dcol_h,
    dslot_h,
    drow_h,
    st_h,
    scol_h,
    sslot_h,
    srow_h,
    pt_h,
    sol_o,
    res_o,
    pos_v,
    x_v,
    x3,
    q_v,
    w_v,
    mass_v,
    land,
    tb,
    xg,
    prod,
    acc,
    got_d,
    got_s,
    pack,
    sel_l,
    sel_s,
    sel_d,
    lcol_v,
    scol_v,
    dcol_v,
    drow_v,
    drow_r,
    part,
    row1,
    rows,
    lrow_m,
    live_m,
    sslot_m,
    srow_m,
    dslot_m,
    drow_m,
    idx,
    spot,
    in_sem,
    tile_sem,
    ix_send,
    ix_recv,
    ix_loc,
    sd_send,
    sd_recv,
    ss_send,
    ss_recv,
    a1_send,
    a1_recv,
):
    a = lax.axis_index("dom")
    b = lax.axis_index("sub")

    def dom_dev(j):
        return {"dom": jnp.bitwise_xor(a, 1 << j)}

    def sub_dev(o):
        return {"sub": lax.rem(b + o, N_SUB)}

    barrier = pltpu.get_barrier_semaphore()
    for j in range(BITS):
        pl.semaphore_signal(barrier, inc=1, device_id=dom_dev(j))
    for o in range(1, N_SUB):
        pl.semaphore_signal(barrier, inc=1, device_id=sub_dev(o))

    small = [
        (pos_h, pos_v),
        (drow_h, drow_v),
        (mass_h, mass_v),
        (lrow_h, lrow_m),
        (live_h, live_m),
        (sslot_h, sslot_m),
        (srow_h, srow_m),
        (dslot_h, dslot_m),
        (lcol_h, lcol_v),
        (scol_h, scol_v),
        (dcol_h, dcol_v),
    ]
    small = [
        pltpu.make_async_copy(src, dst, in_sem.at[i]) for i, (src, dst) in enumerate(small)
    ]
    for copy in small:
        copy.start()
    loads = []
    for src, first in ((lt_h, PAIR_L), (st_h, PAIR_S), (dt_h, PAIR_D), (pt_h, PAIR_P)):
        for start in range(0, src.shape[0], GROUP):
            loads.append(
                pltpu.make_async_copy(
                    src.at[pl.ds(start, GROUP)],
                    land.at[pl.ds(2 * first + start, GROUP)],
                    tile_sem.at[len(loads)],
                )
            )
    for copy in loads[:EARLY]:
        copy.start()

    def dom_copy(p, j):
        return pltpu.make_async_remote_copy(
            src_ref=x_v.at[p],
            dst_ref=got_d.at[p, j],
            send_sem=sd_send.at[p, j],
            recv_sem=sd_recv.at[p, j],
            device_id=dom_dev(j),
        )

    def sub_copy(p, o):
        return pltpu.make_async_remote_copy(
            src_ref=pack.at[p, o - 1],
            dst_ref=got_s.at[p, N_SUB - 1 - o],
            send_sem=ss_send.at[p, o - 1],
            recv_sem=ss_recv.at[p, N_SUB - 1 - o],
            device_id=sub_dev(o),
        )

    def sub_arrival(p, e):
        return pltpu.make_async_remote_copy(
            src_ref=pack.at[p, e],
            dst_ref=got_s.at[p, e],
            send_sem=ss_send.at[p, e],
            recv_sem=ss_recv.at[p, e],
            device_id=sub_dev(e + 1),
        )

    def row_copy(j):
        return pltpu.make_async_remote_copy(
            src_ref=drow_v,
            dst_ref=drow_r.at[j],
            send_sem=ix_send.at[j],
            recv_sem=ix_recv.at[j],
            device_id=dom_dev(j),
        )

    def send(p):
        for j in (1, 3, 0, 2):
            dom_copy(p, j).start()

        def gather(i, carry):
            for s in range(SS):
                block = srow_m[lax.rem(b + i + 1, N_SUB) * SS + s]
                rows = x3[p, block]
                for k in range(DIMS):
                    pack[p, i, k, pl.ds(s, 1), :] = rows[k : k + 1]
            return carry

        lax.fori_loop(0, N_SUB - 1, gather, 0)
        for o in (4, 3, 5, 2, 6, 1, 7):
            sub_copy(p, o).start()

    xg3 = xg.reshape(ROWS_X, 8, TILE)

    def split(base, count, values):
        for k in range(DIMS):
            high = values[k].astype(BF16).astype(F32)
            xg[pl.ds(base * 8 + k, count, stride=8), :] = high
            xg[pl.ds(base * 8 + DIMS + k, count, stride=8), :] = values[k] - high

    def multiply(pair, first, second, slot):
        left = jnp.concatenate(
            [xg3[first], xg3[second]],
            axis=0,
        ).astype(BF16)
        out = jnp.dot(
            jnp.concatenate([left, left], axis=1),
            jnp.concatenate(
                [tb[pair, 0, 0 : 2 * TILE, :], tb[pair, 1, 0 : 2 * TILE, :]], axis=1
            ),
            preferred_element_type=F32,
        )
        prod[pl.ds(pl.multiple_of(slot * 16, 16), 8), :] = out[0:8, 0:TILE]
        prod[pl.ds(pl.multiple_of(slot * 16 + 8, 8), 8), :] = out[8:16, TILE : 2 * TILE]

    def run(first, count):
        def body(i, carry):
            pair = first + i
            multiply(pair, idx[2 * pair], idx[2 * pair + 1], pair)
            return carry

        lax.fori_loop(0, count, body, 0, unroll=True)

    def taken(first, count, k):
        return (
            prod[pl.ds(first * 16 + k, count, stride=8), :]
            + prod[pl.ds(first * 16 + DIMS + k, count, stride=8), :]
        )

    def combine(select, first, count):
        terms = []
        for k in range(DIMS):
            value = taken(first, count, k)
            high = value.astype(BF16)
            rest = value - high.astype(F32)
            middle = rest.astype(BF16)
            terms += [high, middle, (rest - middle.astype(F32)).astype(BF16)]
        out = jnp.dot(
            select[...], jnp.concatenate(terms, axis=1), preferred_element_type=F32
        )
        sums = []
        for k in range(DIMS):
            at = 3 * k * TILE
            sums.append(
                out[:, at + 2 * TILE : at + 3 * TILE]
                + out[:, at + TILE : at + 2 * TILE]
                + out[:, at : at + TILE]
            )
        return sums

    small[0].wait()
    for c in range(NB):
        x3[0, c, 0:DIMS, :] = pos_v[:, c * TILE : (c + 1) * TILE]
    for k in range(DIMS):
        x_v[0, k] = x3[0, :, k, :]
    for copy in small[1:]:
        copy.wait()
    pl.semaphore_wait(barrier, BITS + N_SUB - 1)
    for j in range(BITS):
        row_copy(j).start()
    send(0)
    for copy in loads[EARLY:]:
        copy.start()

    block_ids = lax.broadcasted_iota(jnp.int32, (NB, LT), 0)
    tile_ids = lax.broadcasted_iota(jnp.int32, (NB, LT), 1)
    hit = jnp.logical_and(lcol_v[...] == block_ids, tile_ids < live_m[0])
    sel_l[...] = jnp.where(hit, 1.0, 0.0).astype(BF16)
    sel_s[...] = jnp.where(
        scol_v[...] == lax.broadcasted_iota(jnp.int32, (NB, IFS), 0), 1.0, 0.0
    ).astype(BF16)
    sel_d[...] = jnp.where(
        dcol_v[...] == lax.broadcasted_iota(jnp.int32, (NB, IFD), 0), 1.0, 0.0
    ).astype(BF16)
    xg[...] = jnp.zeros_like(xg)

    def put_local(t, carry):
        idx[t] = lrow_m[t]
        return carry

    def put_sub(t, carry):
        slot = sslot_m[t]
        place = jnp.bitwise_and(jnp.right_shift(slot, 3) - b - 1, N_SUB - 1)
        idx[2 * PAIR_S + t] = BASE_S + place * SS + jnp.bitwise_and(slot, SS - 1)
        return carry

    lax.fori_loop(0, LT, put_local, 0, unroll=8)
    lax.fori_loop(0, IFS, put_sub, 0, unroll=8)

    def convert(i):
        for half in range(2):
            tile = land[2 * i + half]
            high = tile.astype(BF16)
            low = (tile - high.astype(F32)).astype(BF16)
            tb[i, half, 0:TILE, :] = high
            tb[i, half, TILE : 2 * TILE, :] = low

    def arrive(first, count):
        def body(n, carry):
            pltpu.make_async_copy(
                lt_h.at[pl.ds(0, GROUP)],
                land.at[pl.ds(n * GROUP, GROUP)],
                tile_sem.at[n],
            ).wait()
            for i in range(GROUP // 2):
                convert(n * GROUP // 2 + i)
            return carry

        lax.fori_loop(first * 2 // GROUP, (first + count) * 2 // GROUP, body, 0)

    def put_place(t, carry):
        slot = dslot_m[t]
        other = jnp.bitwise_xor(jnp.right_shift(slot, 5), a)
        bit = (
            (other >= 2).astype(jnp.int32)
            + (other >= 4).astype(jnp.int32)
            + (other >= 8).astype(jnp.int32)
        )
        place = a * SD + jnp.bitwise_and(slot, SD - 1)
        spot[0, t] = bit
        spot[1, t] = jnp.right_shift(place, 7)
        spot[2, t] = jnp.bitwise_and(place, TILE - 1)
        return carry

    lax.fori_loop(0, IFD, put_place, 0, unroll=8)

    def put_dom(t, carry):
        bit = spot[0, t]
        block = drow_m[bit, spot[1, t], spot[2, t]]
        idx[2 * PAIR_D + t] = BASE_D + bit * NB + block
        return carry

    part[...] = jnp.zeros_like(part)
    wanted = [(0, 0), (0, 1), (0, 2), (1, 1), (1, 2), (2, 2)]

    moved = pltpu.make_async_copy(drow_r, drow_m, ix_loc)

    def phase(p, first):
        if first:
            arrive(PAIR_L, LT // 2)
        else:
            send(p)
        split(0, NB, [x_v[p, k] for k in range(DIMS)])
        run(PAIR_L, LT // 2)
        if first:
            for j in range(BITS):
                row_copy(j).wait_recv()
            moved.start()
            arrive(PAIR_S, IFS // 2)
        else:

            @pl.when(p == PHASES - 1)
            def _():
                for n, (i, j) in enumerate(wanted):
                    for k in range(DIMS):
                        part[pl.ds(n * DIMS + k, 1), :] = jnp.sum(
                            q_v[i, k] * x_v[j + 1, k], axis=0, keepdims=True
                        )

        for o in (7, 1, 2, 6, 3, 5, 4):
            e = N_SUB - 1 - o
            sub_arrival(p, e).wait_recv()
            split(BASE_S + e * SS, SS, [got_s[p, e, k] for k in range(DIMS)])
        run(PAIR_S, IFS // 2)
        if first:
            arrive(PAIR_D, IFD // 2)
            arrive(PAIR_P, NB // 2)
        inner = combine(sel_l, PAIR_L, LT)
        middle = combine(sel_s, PAIR_S, IFS)
        for k in range(DIMS):
            acc[k] = mass_v[...] * x_v[p, k] + (inner[k] + middle[k])
        if first:
            moved.wait()
            lax.fori_loop(0, IFD, put_dom, 0, unroll=True)
        for j in (0, 2, 1, 3):
            dom_copy(p, j).wait_recv()
            split(BASE_D + j * NB, NB, [got_d[p, j, k] for k in range(DIMS)])
        run(PAIR_D, IFD // 2)
        outer = combine(sel_d, PAIR_D, IFD)

        def smooth():
            split(0, NB, [q_v[p, k] for k in range(DIMS)])

            def body(i, carry):
                multiply(PAIR_P + i, 2 * i, 2 * i + 1, PAIR_P + i)
                return carry

            lax.fori_loop(0, NB // 2, body, 0, unroll=True)
            for k in range(DIMS):
                value = taken(PAIR_P, NB, k)
                x_v[p + 1, k] = value
                x3[p + 1, :, k, :] = value

        if first:
            for k in range(DIMS):
                q_v[0, k] = mass_v[...] * x_v[0, k] - (acc[k] + outer[k])
            smooth()
        else:
            for k in range(DIMS):
                w_v[p - 1, k] = acc[k] + outer[k]

            @pl.when(p < PHASES - 1)
            def _():
                for k in range(DIMS):
                    q_v[p, k] = w_v[p - 1, k] - SHIFT * q_v[p - 1, k]
                smooth()

    def later(p, carry):
        phase(p, False)
        return carry

    phase(0, True)
    lax.fori_loop(1, PHASES, later, 0)
    for k in range(DIMS):
        part[pl.ds(6 * DIMS + k, 1), :] = jnp.sum(
            x_v[3, k] * w_v[2, k], axis=0, keepdims=True
        )
    sums = jnp.sum(part[...], axis=1, keepdims=True)
    eye = lax.broadcasted_iota(jnp.int32, part.shape, 0) == lax.broadcasted_iota(
        jnp.int32, part.shape, 1
    )
    me = a * N_SUB + b
    row1[...] = jnp.sum(jnp.where(eye, sums, 0.0), axis=0, keepdims=True)

    def hops(m):
        return sum((0, 1, 2, 1)[(m >> at) & 3] for at in (1, 3, 5))

    for m in sorted(range(1, N_DOM * N_SUB), key=lambda m: -hops(m)):
        other = jnp.bitwise_xor(me, m)
        pltpu.make_async_remote_copy(
            src_ref=row1,
            dst_ref=rows.at[pl.ds(me, 1)],
            send_sem=a1_send,
            recv_sem=a1_recv,
            device_id={
                "dom": jnp.right_shift(other, 3),
                "sub": jnp.bitwise_and(other, N_SUB - 1),
            },
        ).start()
    rows[pl.ds(me, 1), :] = row1[...]
    everyone = rows.at[pl.ds(0, N_DOM * N_SUB - 1)]
    both = pltpu.make_async_remote_copy(
        src_ref=everyone,
        dst_ref=everyone,
        send_sem=a1_send,
        recv_sem=a1_recv,
        device_id=sub_dev(1),
    )
    both.wait_recv()
    total = jnp.sum(rows[...], axis=0, keepdims=True)

    wide = jnp.broadcast_to(total, (8, TILE))
    values = [wide] + [pltpu.roll(wide, TILE - DIMS * n, 1) for n in range(1, 7)]
    gram = {}
    for (i, j), value in zip(wanted, values):
        gram[i, j] = gram[j, i] = value
    curve = {}
    for j in range(2):
        for i in range(3):
            curve[i, j] = curve[j, i] = gram[i, j + 1] + SHIFT * gram[i, j]
    curve[2, 2] = values[6]

    def form(table, vector):
        out = None
        for i in range(len(vector)):
            for j in range(i, len(vector)):
                term = vector[i] * vector[j] * table[i, j]
                term = term if i == j else 2.0 * term
                out = term if out is None else out + term
        return out

    one = jnp.ones((8, TILE), F32)
    rho = [one]
    along = [one]
    current = gram[0, 0]
    solved = [None] * 3
    for it in range(3):
        step = current / form(curve, along)
        for i, value in enumerate(along):
            moved_by = step * value
            solved[i] = moved_by if solved[i] is None else solved[i] + moved_by
        if it < 2:
            fresh = []
            for i in range(len(along) + 1):
                value = rho[i] if i < len(rho) else None
                if i < len(along):
                    value = value - step * (SHIFT * along[i])
                if i > 0:
                    less = step * along[i - 1]
                    value = -less if value is None else value - less
                fresh.append(value)
            rho = fresh
            following = form(gram, rho)
            ratio = following / current
            along = [
                value + ratio * along[i] if i < len(along) else value
                for i, value in enumerate(rho)
            ]
            current = following
    for k in range(DIMS):
        faired = x_v[0, k]
        left = q_v[0, k]
        for j in range(3):
            scale = solved[j][0:1, k : k + 1]
            faired = faired + scale * x_v[j + 1, k]
            left = left - scale * w_v[j, k]
        sol_o[k] = faired
        res_o[k] = left

    both.wait_send()
    for j in range(BITS):
        row_copy(j).wait_send()
    for p in range(PHASES):
        for j in range(BITS):
            dom_copy(p, j).wait_send()
        for o in range(1, N_SUB):
            sub_copy(p, o).wait_send()


def on_device(
    positions,
    mass,
    local_tiles,
    local_rows,
    local_cols,
    live_tiles,
    dom_tiles,
    dom_cols,
    dom_slots,
    dom_rows,
    sub_tiles,
    sub_cols,
    sub_slots,
    sub_rows,
    precond,
):
    vector = jax.ShapeDtypeStruct((DIMS, NB, TILE), F32)
    dma = pltpu.SemaphoreType.DMA
    solved, left = pl.pallas_call(
        kernel,
        out_shape=(vector, vector),
        in_specs=[pl.BlockSpec(memory_space=pl.ANY)] * 15,
        out_specs=(pl.BlockSpec(memory_space=pltpu.VMEM),) * 2,
        scratch_shapes=[
            pltpu.VMEM((DIMS, NB * TILE), F32),
            pltpu.VMEM((PHASES, DIMS, NB, TILE), F32),
            pltpu.VMEM((PHASES, NB, 8, TILE), F32),
            pltpu.VMEM((3, DIMS, NB, TILE), F32),
            pltpu.VMEM((3, DIMS, NB, TILE), F32),
            pltpu.VMEM((NB, TILE), F32),
            pltpu.VMEM((2 * PAIRS, TILE, TILE), F32),
            pltpu.VMEM((PAIRS, 2, 2 * TILE + 16, TILE), BF16),
            pltpu.VMEM((ROWS_X * 8, TILE), F32),
            pltpu.VMEM((PAIRS * 16, TILE), F32),
            pltpu.VMEM((DIMS, NB, TILE), F32),
            pltpu.VMEM((PHASES, BITS, DIMS, NB, TILE), F32),
            pltpu.VMEM((PHASES, N_SUB - 1, DIMS, SS, TILE), F32),
            pltpu.VMEM((PHASES, N_SUB - 1, DIMS, SS, TILE), F32),
            pltpu.VMEM((NB, LT), BF16),
            pltpu.VMEM((NB, IFS), BF16),
            pltpu.VMEM((NB, IFD), BF16),
            pltpu.VMEM((1, LT), jnp.int32),
            pltpu.VMEM((1, IFS), jnp.int32),
            pltpu.VMEM((1, IFD), jnp.int32),
            pltpu.VMEM((4, TILE), jnp.int32),
            pltpu.VMEM((BITS, 4, TILE), jnp.int32),
            pltpu.VMEM((24, TILE), F32),
            pltpu.VMEM((1, TILE), F32),
            pltpu.VMEM((N_DOM * N_SUB, TILE), F32),
            pltpu.SMEM((LT,), jnp.int32),
            pltpu.SMEM((1,), jnp.int32),
            pltpu.SMEM((IFS,), jnp.int32),
            pltpu.SMEM((N_SUB * SS,), jnp.int32),
            pltpu.SMEM((IFD,), jnp.int32),
            pltpu.SMEM((BITS, 4, TILE), jnp.int32),
            pltpu.SMEM((2 * PAIR_P,), jnp.int32),
            pltpu.SMEM((3, IFD), jnp.int32),
            dma((11,)),
            dma((2 * PAIRS // GROUP,)),
            dma((BITS,)),
            dma((BITS,)),
            dma,
            dma((PHASES, BITS)),
            dma((PHASES, BITS)),
            dma((PHASES, N_SUB - 1)),
            dma((PHASES, N_SUB - 1)),
            dma,
            dma,
        ],
        compiler_params=pltpu.CompilerParams(
            collective_id=0, has_side_effects=True, vmem_limit_bytes=56 * 1024 * 1024
        ),
    )(
        positions,
        mass.reshape(NB, TILE),
        local_tiles,
        local_rows,
        local_cols.reshape(1, LT),
        live_tiles,
        dom_tiles,
        dom_cols.reshape(1, IFD),
        dom_slots,
        dom_rows.reshape(4, TILE),
        sub_tiles,
        sub_cols.reshape(1, IFS),
        sub_slots,
        sub_rows,
        precond,
    )
    return solved.reshape(DIMS, NB * TILE), left.reshape(DIMS, NB * TILE)


def solution(mesh):
    flat = P(("dom", "sub"))
    cube = P(("dom", "sub"), None, None)
    vector = P(None, ("dom", "sub"))
    return jax.shard_map(
        on_device,
        mesh=mesh,
        in_specs=(
            vector,
            flat,
            cube,
            flat,
            flat,
            flat,
            cube,
            flat,
            flat,
            flat,
            cube,
            flat,
            flat,
            flat,
            cube,
        ),
        out_specs=(vector, vector),
        check_vma=False,
    )
```

```python
import functools

import jax
import jax.numpy as jnp
from jax import lax
from jax.experimental import pallas as pl
from jax.experimental.pallas import tpu as pltpu
from jax.sharding import PartitionSpec as P

TILE = 128
DIMS = 3
NB = 32
LT = 64
IFD = 32
IFS = 48
SD = 32
SS = 8
N_DOM = 16
N_SUB = 8
BITS = 4
PHASES = 4
SHIFT = 0.9

PAIR_L = 0
PAIR_S = LT // 2
PAIR_D = PAIR_S + IFS // 2
PAIR_P = PAIR_D + IFD // 2
PAIRS = PAIR_P + NB // 2
GROUP = 16
EARLY = LT // GROUP

BASE_D = NB
BASE_S = NB + BITS * NB
ROWS_X = BASE_S + N_SUB * SS

F32 = jnp.float32
BF16 = jnp.bfloat16


def kernel(
    pos_h,
    mass_h,
    lt_h,
    lrow_h,
    lcol_h,
    live_h,
    dt_h,
    dcol_h,
    dslot_h,
    drow_h,
    st_h,
    scol_h,
    sslot_h,
    srow_h,
    pt_h,
    sol_o,
    res_o,
    pos_v,
    x_v,
    x3,
    q_v,
    w_v,
    mass_v,
    land,
    tb,
    xg,
    prod,
    acc,
    got_d,
    got_s,
    pack,
    sel_l,
    sel_r,
    held,
    lcol_v,
    scol_v,
    dcol_v,
    drow_v,
    drow_r,
    part,
    bent,
    last_v,
    row,
    rows,
    lrow_m,
    live_m,
    sslot_m,
    srow_m,
    dslot_m,
    drow_m,
    scol_m,
    dcol_m,
    idx,
    spot,
    in_sem,
    tile_sem,
    ix_send,
    ix_recv,
    ix_loc,
    sd_send,
    sd_recv,
    ss_send,
    ss_recv,
    row_send,
    row_recv,
):
    a = lax.axis_index("dom")
    b = lax.axis_index("sub")

    def dom_dev(j):
        return {"dom": jnp.bitwise_xor(a, 1 << j)}

    def sub_dev(o):
        return {"sub": lax.rem(b + o, N_SUB)}

    barrier = pltpu.get_barrier_semaphore()
    for m in (1, 2, 3, 4, 8, 12):
        pl.semaphore_signal(barrier, inc=1, device_id={"dom": jnp.bitwise_xor(a, m)})
    for o in range(1, N_SUB):
        pl.semaphore_signal(barrier, inc=1, device_id=sub_dev(o))

    small = [
        (pos_h, pos_v),
        (drow_h, drow_v),
        (mass_h, mass_v),
        (lrow_h, lrow_m),
        (live_h, live_m),
        (sslot_h, sslot_m),
        (srow_h, srow_m),
        (dslot_h, dslot_m),
        (lcol_h, lcol_v),
        (scol_h, scol_v),
        (dcol_h, dcol_v),
        (scol_h, scol_m),
        (dcol_h, dcol_m),
    ]
    small = [
        pltpu.make_async_copy(src, dst, in_sem.at[i]) for i, (src, dst) in enumerate(small)
    ]
    for copy in small:
        copy.start()
    loads = []
    for src, first in ((lt_h, PAIR_L), (st_h, PAIR_S), (dt_h, PAIR_D), (pt_h, PAIR_P)):
        for start in range(0, src.shape[0], GROUP):
            loads.append(
                pltpu.make_async_copy(
                    src.at[pl.ds(start, GROUP)],
                    land.at[pl.ds(2 * first + start, GROUP)],
                    tile_sem.at[len(loads)],
                )
            )
    for copy in loads[:EARLY]:
        copy.start()

    def dom_copy(p, j):
        return pltpu.make_async_remote_copy(
            src_ref=x_v.at[p],
            dst_ref=got_d.at[p, j],
            send_sem=sd_send.at[p, j],
            recv_sem=sd_recv.at[p, j],
            device_id=dom_dev(j),
        )

    def sub_copy(p, o):
        return pltpu.make_async_remote_copy(
            src_ref=pack.at[p, o - 1],
            dst_ref=got_s.at[p, N_SUB - 1 - o],
            send_sem=ss_send.at[p, o - 1],
            recv_sem=ss_recv.at[p, N_SUB - 1 - o],
            device_id=sub_dev(o),
        )

    def sub_arrival(p, e):
        return pltpu.make_async_remote_copy(
            src_ref=pack.at[p, e],
            dst_ref=got_s.at[p, e],
            send_sem=ss_send.at[p, e],
            recv_sem=ss_recv.at[p, e],
            device_id=sub_dev(e + 1),
        )

    def row_copy(j):
        return pltpu.make_async_remote_copy(
            src_ref=drow_v,
            dst_ref=drow_r.at[j],
            send_sem=ix_send.at[j],
            recv_sem=ix_recv.at[j],
            device_id=dom_dev(j),
        )

    def send(p):
        for j in (1, 3, 0, 2):
            dom_copy(p, j).start()

        if isinstance(p, int) and p == 0:
            for copy in small[2:]:
                copy.wait()
        order = (4, 3, 5, 2, 6, 1, 7)
        for n, o in enumerate(order):
            for s in range(SS):
                block = srow_m[lax.rem(b + o, N_SUB) * SS + s]
                values = x3[p, block]
                for k in range(DIMS):
                    pack[p, o - 1, k, pl.ds(s, 1), :] = values[k : k + 1]
            if n:
                sub_copy(p, order[n - 1]).start()
        sub_copy(p, order[-1]).start()

    xg3 = xg.reshape(ROWS_X, 8, TILE)

    def split(base, count, values):
        for k in range(DIMS):
            high = values[k].astype(BF16).astype(F32)
            xg[pl.ds(base * 8 + k, count, stride=8), :] = high
            xg[pl.ds(base * 8 + DIMS + k, count, stride=8), :] = values[k] - high

    def multiply(pair, first, second, slot):
        left = jnp.concatenate(
            [xg3[first], xg3[second]],
            axis=0,
        ).astype(BF16)
        out = jnp.dot(
            jnp.concatenate([left, left], axis=1),
            jnp.concatenate(
                [tb[pair, 0, 0 : 2 * TILE, :], tb[pair, 1, 0 : 2 * TILE, :]], axis=1
            ),
            preferred_element_type=F32,
        )
        prod[pl.ds(pl.multiple_of(slot * 16, 16), 8), :] = out[0:8, 0:TILE]
        prod[pl.ds(pl.multiple_of(slot * 16 + 8, 8), 8), :] = out[8:16, TILE : 2 * TILE]

    def run(first, count):
        def body(i, carry):
            pair = first + i
            multiply(pair, idx[2 * pair], idx[2 * pair + 1], pair)
            return carry

        lax.fori_loop(0, count, body, 0, unroll=True)

    def taken(first, count, k):
        return (
            prod[pl.ds(first * 16 + k, count, stride=8), :]
            + prod[pl.ds(first * 16 + DIMS + k, count, stride=8), :]
        )

    def terms_of(first, count):
        terms = []
        for k in range(DIMS):
            value = taken(first, count, k)
            high = value.astype(BF16)
            rest = value - high.astype(F32)
            middle = rest.astype(BF16)
            terms += [high, middle, (rest - middle.astype(F32)).astype(BF16)]
        return jnp.concatenate(terms, axis=1)

    def combine(select, terms):
        out = jnp.dot(select[...], terms, preferred_element_type=F32)
        sums = []
        for k in range(DIMS):
            at = 3 * k * TILE
            sums.append(
                out[:, at + 2 * TILE : at + 3 * TILE]
                + out[:, at + TILE : at + 2 * TILE]
                + out[:, at : at + TILE]
            )
        return sums

    small[1].wait()
    pl.semaphore_wait(barrier, 6 + N_SUB - 1)
    for j in range(BITS):
        row_copy(j).start()
    small[0].wait()
    for c in range(NB):
        x3[0, c, 0:DIMS, :] = pos_v[:, c * TILE : (c + 1) * TILE]
    for k in range(DIMS):
        x_v[0, k] = x3[0, :, k, :]
    send(0)
    for copy in loads[EARLY:]:
        copy.start()

    block_ids = lax.broadcasted_iota(jnp.int32, (NB, LT), 0)
    tile_ids = lax.broadcasted_iota(jnp.int32, (NB, LT), 1)
    hit = jnp.logical_and(lcol_v[...] == block_ids, tile_ids < live_m[0])
    sel_l[...] = jnp.where(hit, 1.0, 0.0).astype(BF16)
    sel_r[:, 0:IFS] = jnp.where(
        scol_v[...] == lax.broadcasted_iota(jnp.int32, (NB, IFS), 0), 1.0, 0.0
    ).astype(BF16)
    sel_r[:, IFS : IFS + IFD] = jnp.where(
        dcol_v[...] == lax.broadcasted_iota(jnp.int32, (NB, IFD), 0), 1.0, 0.0
    ).astype(BF16)
    xg[...] = jnp.zeros_like(xg)

    def put_local(t, carry):
        idx[t] = lrow_m[t]
        return carry

    def put_sub(t, carry):
        slot = sslot_m[t]
        place = jnp.bitwise_and(jnp.right_shift(slot, 3) - b - 1, N_SUB - 1)
        idx[2 * PAIR_S + t] = BASE_S + place * SS + jnp.bitwise_and(slot, SS - 1)
        return carry

    lax.fori_loop(0, LT, put_local, 0, unroll=8)
    lax.fori_loop(0, IFS, put_sub, 0, unroll=8)

    def convert(i):
        for half in range(2):
            tile = land[2 * i + half]
            high = tile.astype(BF16)
            low = (tile - high.astype(F32)).astype(BF16)
            tb[i, half, 0:TILE, :] = high
            tb[i, half, TILE : 2 * TILE, :] = low

    def arrive(first, count):
        def body(n, carry):
            pltpu.make_async_copy(
                lt_h.at[pl.ds(0, GROUP)],
                land.at[pl.ds(n * GROUP, GROUP)],
                tile_sem.at[n],
            ).wait()
            for i in range(GROUP // 2):
                convert(n * GROUP // 2 + i)
            return carry

        lax.fori_loop(first * 2 // GROUP, (first + count) * 2 // GROUP, body, 0)

    def put_place(t, carry):
        slot = dslot_m[t]
        other = jnp.bitwise_xor(jnp.right_shift(slot, 5), a)
        bit = (
            (other >= 2).astype(jnp.int32)
            + (other >= 4).astype(jnp.int32)
            + (other >= 8).astype(jnp.int32)
        )
        place = a * SD + jnp.bitwise_and(slot, SD - 1)
        spot[0, t] = bit
        spot[1, t] = jnp.right_shift(place, 7)
        spot[2, t] = jnp.bitwise_and(place, TILE - 1)
        return carry

    lax.fori_loop(0, IFD, put_place, 0, unroll=8)

    def put_dom(t, carry):
        bit = spot[0, t]
        block = drow_m[bit, spot[1, t], spot[2, t]]
        idx[2 * PAIR_D + t] = BASE_D + bit * NB + block
        return carry

    part[...] = jnp.zeros_like(part)
    wanted = [(0, 0), (0, 1), (0, 2), (1, 1), (1, 2), (2, 2)]
    moved = pltpu.make_async_copy(drow_r, drow_m, ix_loc)
    me = a * N_SUB + b
    count = N_DOM * N_SUB

    def hops(m):
        return sum((0, 1, 2, 1)[(m >> at) & 3] for at in (1, 3, 5))

    def row_to(which, m):
        other = jnp.bitwise_xor(me, m)
        return pltpu.make_async_remote_copy(
            src_ref=row.at[which],
            dst_ref=rows.at[which, pl.ds(me, 1)],
            send_sem=row_send.at[which],
            recv_sem=row_recv.at[which],
            device_id={
                "dom": jnp.right_shift(other, 3),
                "sub": jnp.bitwise_and(other, N_SUB - 1),
            },
        )

    def row_all(which):
        everyone = rows.at[which, pl.ds(0, count - 1)]
        return pltpu.make_async_remote_copy(
            src_ref=everyone,
            dst_ref=everyone,
            send_sem=row_send.at[which],
            recv_sem=row_recv.at[which],
            device_id=sub_dev(1),
        )

    def to_row(which, table):
        sums = jnp.sum(table, axis=1, keepdims=True)
        eye = lax.broadcasted_iota(jnp.int32, table.shape, 0) == lax.broadcasted_iota(
            jnp.int32, table.shape, 1
        )
        value = jnp.sum(jnp.where(eye, sums, 0.0), axis=0, keepdims=True)
        row[which] = value
        rows[which, pl.ds(me, 1), :] = value

    def early_rows():
        for n, (i, j) in enumerate(wanted):
            for k in range(DIMS):
                part[pl.ds(n * DIMS + k, 1), :] = jnp.sum(
                    q_v[i, k] * x_v[j + 1, k], axis=0, keepdims=True
                )
        to_row(0, part[...])

        def body(i, carry):
            row_to(0, i + 1).start()
            return carry

        lax.fori_loop(0, count - 1, body, 0, unroll=4)

    def met(p, first, count, columns):
        total = None
        for t in range(count):
            at = (2 * first + t) * 8
            term = x3[p, columns[0, t]] * prod[at : at + 8, :]
            total = term if total is None else total + term
        return total

    def phase(p, first, last):
        if first:
            arrive(PAIR_L, LT // 2)
        else:
            send(p)
        split(0, NB, [x_v[p, k] for k in range(DIMS)])
        run(PAIR_L, LT // 2)
        if first:
            for j in range(BITS):
                row_copy(j).wait_recv()
            moved.start()
            arrive(PAIR_S, IFS // 2)
        inner = combine(sel_l, terms_of(PAIR_L, LT))
        for k in range(DIMS):
            acc[k] = mass_v[...] * x_v[p, k] + inner[k]
        if last:
            early_rows()
            for k in range(DIMS):
                x3[p, :, DIMS + k, :] = x_v[p, k]
        for o in (7, 1, 2, 6, 3, 5, 4):
            e = N_SUB - 1 - o
            sub_arrival(p, e).wait_recv()
            split(BASE_S + e * SS, SS, [got_s[p, e, k] for k in range(DIMS)])
        run(PAIR_S, IFS // 2)
        if first:
            arrive(PAIR_D, IFD // 2)
            arrive(PAIR_P, NB // 2)
        held[...] = terms_of(PAIR_S, IFS)
        if last:
            bent[...] = met(p, PAIR_S, IFS, scol_m)
            for k in range(DIMS):
                bent[k : k + 1, :] += jnp.sum(
                    acc[k] * x_v[p, k], axis=0, keepdims=True
                )
        if first:
            moved.wait()
            lax.fori_loop(0, IFD, put_dom, 0, unroll=True)
        for j in (0, 2, 1, 3):
            dom_copy(p, j).wait_recv()
            split(BASE_D + j * NB, NB, [got_d[p, j, k] for k in range(DIMS)])
        run(PAIR_D, IFD // 2)
        if last:
            whole = bent[...] + met(p, PAIR_D, IFD, dcol_m)
            to_row(1, whole[0:DIMS] + whole[DIMS : 2 * DIMS])
            for m in sorted(range(1, count), key=lambda m: -hops(m)):
                row_to(1, m).start()
        outer = combine(
            sel_r, jnp.concatenate([held[...], terms_of(PAIR_D, IFD)], axis=0)
        )
        for k in range(DIMS):
            value = acc[k] + outer[k]
            if first:
                q_v[0, k] = mass_v[...] * x_v[0, k] - value
            else:
                w_v[p - 1, k] = value
                if not last:
                    q_v[p, k] = value - SHIFT * q_v[p - 1, k]
        if not last:
            split(0, NB, [q_v[p, k] for k in range(DIMS)])
            for i in range(NB // 2):
                multiply(PAIR_P + i, 2 * i, 2 * i + 1, PAIR_P + i)
            for k in range(DIMS):
                value = taken(PAIR_P, NB, k)
                x_v[p + 1, k] = value
                x3[p + 1, :, k, :] = value

    def later(p, carry):
        phase(p, False, False)
        return carry

    phase(0, True, False)
    lax.fori_loop(1, PHASES - 1, later, 0)
    phase(PHASES - 1, False, True)

    row_all(0).wait_recv()
    wide = jnp.broadcast_to(jnp.sum(rows[0], axis=0, keepdims=True), (8, TILE))
    values = [wide] + [pltpu.roll(wide, TILE - DIMS * n, 1) for n in range(1, 6)]
    gram = {}
    for (i, j), value in zip(wanted, values):
        gram[i, j] = gram[j, i] = value
    curve = {}
    for j in range(2):
        for i in range(3):
            curve[i, j] = curve[j, i] = gram[i, j + 1] + SHIFT * gram[i, j]

    def form(table, vector):
        out = None
        for i in range(len(vector)):
            for j in range(i, len(vector)):
                if (i, j) in table:
                    term = vector[i] * vector[j] * table[i, j]
                    term = term if i == j else 2.0 * term
                    out = term if out is None else out + term
        return out

    one = jnp.ones((8, TILE), F32)
    rho = [one]
    along = [one]
    current = gram[0, 0]
    solved = []
    for it in range(2):
        step = current / form(curve, along)
        for i, value in enumerate(along):
            if i < len(solved):
                solved[i] = solved[i] + step * value
            else:
                solved.append(step * value)
        fresh = []
        for i in range(len(along) + 1):
            value = rho[i] if i < len(rho) else None
            if i < len(along):
                value = value - step * (SHIFT * along[i])
            if i > 0:
                less = step * along[i - 1]
                value = -less if value is None else value - less
            fresh.append(value)
        rho = fresh
        following = form(gram, rho)
        ratio = following / current
        along = [
            value + ratio * along[i] if i < len(along) else value
            for i, value in enumerate(rho)
        ]
        current = following
    known = form(curve, along)
    square = along[2] * along[2]
    for k in range(DIMS):
        faired, left = x_v[0, k], q_v[0, k]
        turn, lift = None, None
        for j in range(3):
            scale = along[j][0:1, k : k + 1]
            turn = scale * x_v[j + 1, k] if j == 0 else turn + scale * x_v[j + 1, k]
            lift = scale * w_v[j, k] if j == 0 else lift + scale * w_v[j, k]
            if j < 2:
                scale = solved[j][0:1, k : k + 1]
                faired = faired + scale * x_v[j + 1, k]
                left = left - scale * w_v[j, k]
        last_v[0, k] = faired
        last_v[1, k] = turn
        last_v[2, k] = left
        last_v[3, k] = lift
    row_all(1).wait_recv()
    step = current / (known + square * jnp.sum(rows[1], axis=0, keepdims=True))
    for k in range(DIMS):
        scale = step[0:1, k : k + 1]
        sol_o[k] = last_v[0, k] + scale * last_v[1, k]
        res_o[k] = last_v[2, k] - scale * last_v[3, k]

    for which in range(2):
        row_all(which).wait_send()
    for j in range(BITS):
        row_copy(j).wait_send()
    for p in range(PHASES):
        for j in range(BITS):
            dom_copy(p, j).wait_send()
        for o in range(1, N_SUB):
            sub_copy(p, o).wait_send()


def on_device(
    positions,
    mass,
    local_tiles,
    local_rows,
    local_cols,
    live_tiles,
    dom_tiles,
    dom_cols,
    dom_slots,
    dom_rows,
    sub_tiles,
    sub_cols,
    sub_slots,
    sub_rows,
    precond,
):
    vector = jax.ShapeDtypeStruct((DIMS, NB, TILE), F32)
    dma = pltpu.SemaphoreType.DMA
    solved, left = pl.pallas_call(
        kernel,
        out_shape=(pltpu.VMEM((DIMS, NB, TILE), F32),) * 2,
        in_specs=[pl.BlockSpec(memory_space=pl.ANY)] * 15,
        out_specs=(pl.BlockSpec(memory_space=pltpu.VMEM),) * 2,
        scratch_shapes=[
            pltpu.VMEM((DIMS, NB * TILE), F32),
            pltpu.VMEM((PHASES, DIMS, NB, TILE), F32),
            pltpu.VMEM((PHASES, NB, 8, TILE), F32),
            pltpu.VMEM((3, DIMS, NB, TILE), F32),
            pltpu.VMEM((3, DIMS, NB, TILE), F32),
            pltpu.VMEM((NB, TILE), F32),
            pltpu.VMEM((2 * PAIRS, TILE, TILE), F32),
            pltpu.VMEM((PAIRS, 2, 2 * TILE + 16, TILE), BF16),
            pltpu.VMEM((ROWS_X * 8, TILE), F32),
            pltpu.VMEM((PAIRS * 16, TILE), F32),
            pltpu.VMEM((DIMS, NB, TILE), F32),
            pltpu.VMEM((PHASES, BITS, DIMS, NB, TILE), F32),
            pltpu.VMEM((PHASES, N_SUB - 1, DIMS, SS, TILE), F32),
            pltpu.VMEM((PHASES, N_SUB - 1, DIMS, SS, TILE), F32),
            pltpu.VMEM((NB, LT), BF16),
            pltpu.VMEM((NB, IFS + IFD), BF16),
            pltpu.VMEM((IFS, 9 * TILE), BF16),
            pltpu.VMEM((1, LT), jnp.int32),
            pltpu.VMEM((1, IFS), jnp.int32),
            pltpu.VMEM((1, IFD), jnp.int32),
            pltpu.VMEM((4, TILE), jnp.int32),
            pltpu.VMEM((BITS, 4, TILE), jnp.int32),
            pltpu.VMEM((24, TILE), F32),
            pltpu.VMEM((8, TILE), F32),
            pltpu.VMEM((4, DIMS, NB, TILE), F32),
            pltpu.VMEM((2, 1, TILE), F32),
            pltpu.VMEM((2, N_DOM * N_SUB, TILE), F32),
            pltpu.SMEM((LT,), jnp.int32),
            pltpu.SMEM((1,), jnp.int32),
            pltpu.SMEM((IFS,), jnp.int32),
            pltpu.SMEM((N_SUB * SS,), jnp.int32),
            pltpu.SMEM((IFD,), jnp.int32),
            pltpu.SMEM((BITS, 4, TILE), jnp.int32),
            pltpu.SMEM((1, IFS), jnp.int32),
            pltpu.SMEM((1, IFD), jnp.int32),
            pltpu.SMEM((2 * PAIR_P,), jnp.int32),
            pltpu.SMEM((3, IFD), jnp.int32),
            dma((13,)),
            dma((2 * PAIRS // GROUP,)),
            dma((BITS,)),
            dma((BITS,)),
            dma,
            dma((PHASES, BITS)),
            dma((PHASES, BITS)),
            dma((PHASES, N_SUB - 1)),
            dma((PHASES, N_SUB - 1)),
            dma((2,)),
            dma((2,)),
        ],
        compiler_params=pltpu.CompilerParams(
            collective_id=0, has_side_effects=True, vmem_limit_bytes=56 * 1024 * 1024
        ),
    )(
        positions,
        mass.reshape(NB, TILE),
        local_tiles,
        local_rows,
        local_cols.reshape(1, LT),
        live_tiles,
        dom_tiles,
        dom_cols.reshape(1, IFD),
        dom_slots,
        dom_rows.reshape(4, TILE),
        sub_tiles,
        sub_cols.reshape(1, IFS),
        sub_slots,
        sub_rows,
        precond,
    )
    return solved.reshape(DIMS, NB * TILE), left.reshape(DIMS, NB * TILE)


def solution(mesh):
    flat = P(("dom", "sub"))
    cube = P(("dom", "sub"), None, None)
    vector = P(None, ("dom", "sub"))
    return jax.shard_map(
        on_device,
        mesh=mesh,
        in_specs=(
            vector,
            flat,
            cube,
            flat,
            flat,
            flat,
            cube,
            flat,
            flat,
            flat,
            cube,
            flat,
            flat,
            flat,
            cube,
        ),
        out_specs=(vector, vector),
        check_vma=False,
    )
```

```python
import functools

import jax
import jax.numpy as jnp
from jax import lax
from jax.experimental import pallas as pl
from jax.experimental.pallas import tpu as pltpu
from jax.sharding import PartitionSpec as P

TILE = 128
DIMS = 3
NB = 32
LT = 64
IFD = 32
IFS = 48
SD = 32
SS = 8
N_DOM = 16
N_SUB = 8
BITS = 4
PHASES = 4
SHIFT = 0.9

PAIR_L = 0
PAIR_S = LT // 2
PAIR_D = PAIR_S + IFS // 2
PAIR_P = PAIR_D + IFD // 2
PAIRS = PAIR_P + NB // 2
GROUP = 16
EARLY = LT // GROUP

FAR = (4, 5, 6, 7)
NEAR = (2, 3, 1)
NEAR_TILES = IFS - len(FAR) * SS

BASE_D = NB
BASE_S = NB + BITS * NB
ROWS_X = BASE_S + N_SUB * SS

F32 = jnp.float32
BF16 = jnp.bfloat16


def kernel(
    pos_h,
    mass_h,
    lt_h,
    lrow_h,
    lcol_h,
    live_h,
    dt_h,
    dcol_h,
    dslot_h,
    drow_h,
    st_h,
    scol_h,
    sslot_h,
    srow_h,
    pt_h,
    sol_o,
    res_o,
    pos_v,
    x_v,
    x3,
    q_v,
    w_v,
    mass_v,
    land,
    tb,
    xg,
    prod,
    acc,
    got_d,
    got_s,
    pack,
    sel_l,
    sel_r,
    held,
    lcol_v,
    scol_v,
    dcol_v,
    sslot_v,
    tab_v,
    drow_v,
    drow_r,
    part,
    bent,
    last_v,
    row,
    rows,
    lrow_m,
    live_m,
    srow_m,
    dslot_m,
    drow_m,
    dcol_m,
    tab_m,
    idx,
    spot,
    in_sem,
    tile_sem,
    ix_send,
    ix_recv,
    ix_loc,
    tab_sem,
    sd_send,
    sd_recv,
    ss_send,
    ss_recv,
    row_send,
    row_recv,
):
    a = lax.axis_index("dom")
    b = lax.axis_index("sub")

    def dom_dev(j):
        return {"dom": jnp.bitwise_xor(a, 1 << j)}

    def sub_dev(m):
        return {"sub": jnp.bitwise_xor(b, m)}

    small = [
        (pos_h, pos_v),
        (drow_h, drow_v),
        (mass_h, mass_v),
        (lrow_h, lrow_m),
        (live_h, live_m),
        (sslot_h, sslot_v),
        (srow_h, srow_m),
        (dslot_h, dslot_m),
        (lcol_h, lcol_v),
        (scol_h, scol_v),
        (dcol_h, dcol_v),
        (dcol_h, dcol_m),
    ]
    small = [
        pltpu.make_async_copy(src, dst, in_sem.at[i]) for i, (src, dst) in enumerate(small)
    ]
    for copy in small:
        copy.start()
    loads = []
    for src, first in ((lt_h, PAIR_L), (st_h, PAIR_S), (dt_h, PAIR_D), (pt_h, PAIR_P)):
        for start in range(0, src.shape[0], GROUP):
            loads.append(
                pltpu.make_async_copy(
                    src.at[pl.ds(start, GROUP)],
                    land.at[pl.ds(2 * first + start, GROUP)],
                    tile_sem.at[len(loads)],
                )
            )
    barrier = pltpu.get_barrier_semaphore()
    for m in (1, 2, 3, 4, 8, 12):
        pl.semaphore_signal(barrier, inc=1, device_id={"dom": jnp.bitwise_xor(a, m)})
    for o in range(1, N_SUB):
        pl.semaphore_signal(barrier, inc=1, device_id=sub_dev(o))

    for copy in loads[:EARLY]:
        copy.start()

    def dom_copy(p, j):
        return pltpu.make_async_remote_copy(
            src_ref=x_v.at[p],
            dst_ref=got_d.at[p, j],
            send_sem=sd_send.at[p, j],
            recv_sem=sd_recv.at[p, j],
            device_id=dom_dev(j),
        )

    def sub_copy(p, m):
        return pltpu.make_async_remote_copy(
            src_ref=pack.at[p, m - 1],
            dst_ref=got_s.at[p, m - 1],
            send_sem=ss_send.at[p, m - 1],
            recv_sem=ss_recv.at[p, m - 1],
            device_id=sub_dev(m),
        )

    def row_copy(j):
        return pltpu.make_async_remote_copy(
            src_ref=drow_v,
            dst_ref=drow_r.at[j],
            send_sem=ix_send.at[j],
            recv_sem=ix_recv.at[j],
            device_id=dom_dev(j),
        )

    def send(p):
        for j in (1, 3):
            dom_copy(p, j).start()

        if isinstance(p, int) and p == 0:
            for copy in small[2:]:
                copy.wait()
        order = FAR + NEAR
        for n, o in enumerate(order):
            for s in range(SS):
                block = srow_m[jnp.bitwise_xor(b, o) * SS + s]
                values = x3[p, block]
                for k in range(DIMS):
                    pack[p, o - 1, k, pl.ds(s, 1), :] = values[k : k + 1]
            if n:
                sub_copy(p, order[n - 1]).start()
        sub_copy(p, order[-1]).start()
        for j in (0, 2):
            dom_copy(p, j).start()

    xg3 = xg.reshape(ROWS_X, 8, TILE)

    def split(base, count, values):
        for k in range(DIMS):
            high = values[k].astype(BF16).astype(F32)
            xg[pl.ds(base * 8 + k, count, stride=8), :] = high
            xg[pl.ds(base * 8 + DIMS + k, count, stride=8), :] = values[k] - high

    def multiply(slot, one, two, first, second):
        left = jnp.concatenate([xg3[first], xg3[second]], axis=0).astype(BF16)
        out = jnp.dot(
            jnp.concatenate([left, left], axis=1),
            jnp.concatenate(
                [tb[one, 0 : 2 * TILE, :], tb[two, 0 : 2 * TILE, :]], axis=1
            ),
            preferred_element_type=F32,
        )
        prod[slot * 16 : slot * 16 + 8, :] = out[0:8, 0:TILE]
        prod[slot * 16 + 8 : slot * 16 + 16, :] = out[8:16, TILE : 2 * TILE]

    def run(first, count):
        for slot in range(first, first + count):
            one = 2 * slot
            multiply(slot, one, one + 1, idx[one], idx[one + 1])

    def run_sub(first, last):
        for t in range(first, last, 2):
            multiply(
                PAIR_S + t // 2,
                2 * PAIR_S + tab_m[0, t],
                2 * PAIR_S + tab_m[0, t + 1],
                tab_m[1, t],
                tab_m[1, t + 1],
            )

    def taken(first, count, k):
        return (
            prod[pl.ds(first * 8 + k, count, stride=8), :]
            + prod[pl.ds(first * 8 + DIMS + k, count, stride=8), :]
        )

    def terms_of(first, count):
        terms = []
        for k in range(DIMS):
            value = taken(first, count, k)
            high = value.astype(BF16)
            terms += [high, (value - high.astype(F32)).astype(BF16)]
        return jnp.concatenate(terms, axis=1)

    def combine(select, terms):
        out = jnp.dot(select[...], terms, preferred_element_type=F32)
        sums = []
        for k in range(DIMS):
            at = 2 * k * TILE
            sums.append(out[:, at + TILE : at + 2 * TILE] + out[:, at : at + TILE])
        return sums

    small[1].wait()
    pl.semaphore_wait(barrier, 6 + N_SUB - 1)
    for j in range(BITS):
        row_copy(j).start()
    small[0].wait()
    for c in range(NB):
        x3[0, c, 0:DIMS, :] = pos_v[:, c * TILE : (c + 1) * TILE]
    for k in range(DIMS):
        x_v[0, k] = x3[0, :, k, :]
    send(0)
    for copy in loads[EARLY:]:
        copy.start()

    block_ids = lax.broadcasted_iota(jnp.int32, (NB, LT), 0)
    tile_ids = lax.broadcasted_iota(jnp.int32, (NB, LT), 1)
    hit = jnp.logical_and(lcol_v[...] == block_ids, tile_ids < live_m[0])
    sel_l[...] = jnp.where(hit, 1.0, 0.0).astype(BF16)
    square = (IFS, IFS)
    down = lax.broadcasted_iota(jnp.int32, square, 0)
    across = lax.broadcasted_iota(jnp.int32, square, 1)

    def stand(values):
        return jnp.sum(
            jnp.where(down == across, values.astype(F32), 0.0), axis=1, keepdims=True
        )

    slot = sslot_v[...]
    apart = jnp.bitwise_xor(jnp.right_shift(slot, 3), b)
    place = BASE_S + (apart - 1) * SS + jnp.bitwise_and(slot, SS - 1)
    key = lax.broadcasted_iota(jnp.int32, (1, IFS), 1) + jnp.where(
        apart >= 4, TILE, 0
    )
    keys = stand(key)
    rank = jnp.sum(
        jnp.where(key.astype(F32) < keys, 1.0, 0.0), axis=1, keepdims=True
    )
    chosen = jnp.where(rank == across.astype(F32), 1.0, 0.0)
    tab_v[...] = jnp.zeros_like(tab_v)
    ranges = (IFS, ROWS_X, NB)
    for n, values in enumerate((down.astype(F32), stand(place), stand(scol_v[...]))):
        line = jnp.sum(chosen * values, axis=0, keepdims=True).astype(jnp.int32)
        line = jnp.clip(line, 0, ranges[n] - 1)
        tab_v[n : n + 1, 0:IFS] = line
    tabled = pltpu.make_async_copy(tab_v, tab_m, tab_sem)
    tabled.start()
    sel_r[:, 0:IFS] = jnp.where(
        line == lax.broadcasted_iota(jnp.int32, (NB, IFS), 0), 1.0, 0.0
    ).astype(BF16)
    sel_r[:, IFS : IFS + IFD] = jnp.where(
        dcol_v[...] == lax.broadcasted_iota(jnp.int32, (NB, IFD), 0), 1.0, 0.0
    ).astype(BF16)
    xg[...] = jnp.zeros_like(xg)

    def put_local(t, carry):
        idx[t] = lrow_m[t]
        return carry

    lax.fori_loop(0, LT, put_local, 0, unroll=8)

    def convert(i):
        for half in range(2):
            tile = land[2 * i + half]
            high = tile.astype(BF16)
            low = (tile - high.astype(F32)).astype(BF16)
            tb[2 * i + half, 0:TILE, :] = high
            tb[2 * i + half, TILE : 2 * TILE, :] = low

    def arrive(first, count):
        def body(n, carry):
            pltpu.make_async_copy(
                lt_h.at[pl.ds(0, GROUP)],
                land.at[pl.ds(n * GROUP, GROUP)],
                tile_sem.at[n],
            ).wait()
            for i in range(GROUP // 2):
                convert(n * GROUP // 2 + i)
            return carry

        lax.fori_loop(first * 2 // GROUP, (first + count) * 2 // GROUP, body, 0)

    def put_place(t, carry):
        slot = dslot_m[t]
        other = jnp.bitwise_xor(jnp.right_shift(slot, 5), a)
        bit = (
            (other >= 2).astype(jnp.int32)
            + (other >= 4).astype(jnp.int32)
            + (other >= 8).astype(jnp.int32)
        )
        place = a * SD + jnp.bitwise_and(slot, SD - 1)
        spot[0, t] = bit
        spot[1, t] = jnp.right_shift(place, 7)
        spot[2, t] = jnp.bitwise_and(place, TILE - 1)
        return carry

    lax.fori_loop(0, IFD, put_place, 0, unroll=8)

    def put_dom(t, carry):
        bit = spot[0, t]
        block = drow_m[bit, spot[1, t], spot[2, t]]
        idx[2 * PAIR_D + t] = BASE_D + bit * NB + block
        return carry

    part[...] = jnp.zeros_like(part)
    wanted = [(0, 0), (0, 1), (0, 2), (1, 1), (1, 2), (2, 2)]
    moved = pltpu.make_async_copy(drow_r, drow_m, ix_loc)
    me = a * N_SUB + b
    count = N_DOM * N_SUB

    def hops(m):
        return sum((0, 1, 2, 1)[(m >> at) & 3] for at in (1, 3, 5))

    def row_to(which, m):
        other = jnp.bitwise_xor(me, m)
        return pltpu.make_async_remote_copy(
            src_ref=row.at[which],
            dst_ref=rows.at[which, pl.ds(me, 1)],
            send_sem=row_send.at[which],
            recv_sem=row_recv.at[which],
            device_id={
                "dom": jnp.right_shift(other, 3),
                "sub": jnp.bitwise_and(other, N_SUB - 1),
            },
        )

    def row_all(which):
        everyone = rows.at[which, pl.ds(0, count - 1)]
        return pltpu.make_async_remote_copy(
            src_ref=everyone,
            dst_ref=everyone,
            send_sem=row_send.at[which],
            recv_sem=row_recv.at[which],
            device_id=sub_dev(1),
        )

    def to_row(which, table):
        sums = jnp.sum(table, axis=1, keepdims=True)
        eye = lax.broadcasted_iota(jnp.int32, table.shape, 0) == lax.broadcasted_iota(
            jnp.int32, table.shape, 1
        )
        value = jnp.sum(jnp.where(eye, sums, 0.0), axis=0, keepdims=True)
        row[which] = value
        rows[which, pl.ds(me, 1), :] = value

    def early_rows():
        for n, (i, j) in enumerate(wanted):
            for k in range(DIMS):
                part[pl.ds(n * DIMS + k, 1), :] = jnp.sum(
                    q_v[i, k] * x_v[j + 1, k], axis=0, keepdims=True
                )
        to_row(0, part[...])

        def body(i, carry):
            row_to(0, i + 1).start()
            return carry

        lax.fori_loop(0, count - 1, body, 0, unroll=4)

    def met(p, first, count, table, line, start=0):
        total = None
        for t in range(count):
            at = (first + t) * 8
            term = x3[p, table[line, start + t]] * prod[at : at + 8, :]
            total = term if total is None else total + term
        return total

    def phase(p, first, last):
        if first:
            arrive(PAIR_L, LT // 2)
        else:
            send(p)
        split(0, NB, [x_v[p, k] for k in range(DIMS)])
        run(PAIR_L, LT // 2)
        if first:
            for j in range(BITS):
                row_copy(j).wait_recv()
            moved.start()
            arrive(PAIR_S, IFS // 2)
        inner = combine(sel_l, terms_of(2 * PAIR_L, LT))
        for k in range(DIMS):
            acc[k] = mass_v[...] * x_v[p, k] + inner[k]
        if last:
            early_rows()
            for k in range(DIMS):
                x3[p, :, DIMS + k, :] = x_v[p, k]
        def take(ms):
            for m in ms:
                sub_copy(p, m).wait_recv()
                split(
                    BASE_S + (m - 1) * SS, SS, [got_s[p, m - 1, k] for k in range(DIMS)]
                )

        if first:
            tabled.wait()
        take(NEAR[::-1])
        run_sub(0, NEAR_TILES)
        held[...] = terms_of(2 * PAIR_S, NEAR_TILES)
        if last:
            bent[...] = met(p, 2 * PAIR_S, NEAR_TILES, tab_m, 2)
            for k in range(DIMS):
                bent[k : k + 1, :] += jnp.sum(
                    acc[k] * x_v[p, k], axis=0, keepdims=True
                )
        if first:
            arrive(PAIR_D, IFD // 2)
            arrive(PAIR_P, NB // 2)
        take(FAR)
        run_sub(NEAR_TILES, IFS)
        if first:
            moved.wait()
            lax.fori_loop(0, IFD, put_dom, 0, unroll=True)
        for j in (0, 2, 1, 3):
            dom_copy(p, j).wait_recv()
            split(BASE_D + j * NB, NB, [got_d[p, j, k] for k in range(DIMS)])
        run(PAIR_D, IFD // 2)
        if last:
            whole = bent[...] + met(
                p, 2 * PAIR_S + NEAR_TILES, IFS - NEAR_TILES, tab_m, 2, NEAR_TILES
            )
            whole = whole + met(p, 2 * PAIR_D, IFD, dcol_m, 0)
            to_row(1, whole[0:DIMS] + whole[DIMS : 2 * DIMS])
            for m in sorted(range(1, count), key=lambda m: -hops(m)):
                row_to(1, m).start()
        outer = combine(
            sel_r,
            jnp.concatenate(
                [
                    held[...],
                    terms_of(2 * PAIR_S + NEAR_TILES, IFS - NEAR_TILES + IFD),
                ],
                axis=0,
            ),

        )
        for k in range(DIMS):
            value = acc[k] + outer[k]
            if first:
                q_v[0, k] = mass_v[...] * x_v[0, k] - value
            else:
                w_v[p - 1, k] = value
                if not last:
                    q_v[p, k] = value - SHIFT * q_v[p - 1, k]
        if not last:
            split(0, NB, [q_v[p, k] for k in range(DIMS)])
            for i in range(NB // 2):
                one = 2 * (PAIR_P + i)
                multiply(PAIR_P + i, one, one + 1, 2 * i, 2 * i + 1)
            for k in range(DIMS):
                value = taken(2 * PAIR_P, NB, k)
                x_v[p + 1, k] = value
                x3[p + 1, :, k, :] = value

    def later(p, carry):
        phase(p, False, False)
        return carry

    phase(0, True, False)
    lax.fori_loop(1, PHASES - 1, later, 0)
    phase(PHASES - 1, False, True)

    row_all(0).wait_recv()
    wide = jnp.broadcast_to(jnp.sum(rows[0], axis=0, keepdims=True), (8, TILE))
    values = [wide] + [pltpu.roll(wide, TILE - DIMS * n, 1) for n in range(1, 6)]
    gram = {}
    for (i, j), value in zip(wanted, values):
        gram[i, j] = gram[j, i] = value
    curve = {}
    for j in range(2):
        for i in range(3):
            curve[i, j] = curve[j, i] = gram[i, j + 1] + SHIFT * gram[i, j]

    def form(table, vector):
        out = None
        for i in range(len(vector)):
            for j in range(i, len(vector)):
                if (i, j) in table:
                    term = vector[i] * vector[j] * table[i, j]
                    term = term if i == j else 2.0 * term
                    out = term if out is None else out + term
        return out

    one = jnp.ones((8, TILE), F32)
    rho = [one]
    along = [one]
    current = gram[0, 0]
    solved = []
    for it in range(2):
        step = current / form(curve, along)
        for i, value in enumerate(along):
            if i < len(solved):
                solved[i] = solved[i] + step * value
            else:
                solved.append(step * value)
        fresh = []
        for i in range(len(along) + 1):
            value = rho[i] if i < len(rho) else None
            if i < len(along):
                value = value - step * (SHIFT * along[i])
            if i > 0:
                less = step * along[i - 1]
                value = -less if value is None else value - less
            fresh.append(value)
        rho = fresh
        following = form(gram, rho)
        ratio = following / current
        along = [
            value + ratio * along[i] if i < len(along) else value
            for i, value in enumerate(rho)
        ]
        current = following
    known = form(curve, along)
    square = along[2] * along[2]
    for k in range(DIMS):
        faired, left = x_v[0, k], q_v[0, k]
        turn, lift = None, None
        for j in range(3):
            scale = along[j][0:1, k : k + 1]
            turn = scale * x_v[j + 1, k] if j == 0 else turn + scale * x_v[j + 1, k]
            lift = scale * w_v[j, k] if j == 0 else lift + scale * w_v[j, k]
            if j < 2:
                scale = solved[j][0:1, k : k + 1]
                faired = faired + scale * x_v[j + 1, k]
                left = left - scale * w_v[j, k]
        last_v[0, k] = faired
        last_v[1, k] = turn
        last_v[2, k] = left
        last_v[3, k] = lift
    row_all(1).wait_recv()
    step = current / (known + square * jnp.sum(rows[1], axis=0, keepdims=True))
    for k in range(DIMS):
        scale = step[0:1, k : k + 1]
        sol_o[k] = last_v[0, k] + scale * last_v[1, k]
        res_o[k] = last_v[2, k] - scale * last_v[3, k]

    for which in range(2):
        row_all(which).wait_send()
    for j in range(BITS):
        row_copy(j).wait_send()
    for p in range(PHASES):
        for j in range(BITS):
            dom_copy(p, j).wait_send()
        for o in range(1, N_SUB):
            sub_copy(p, o).wait_send()


def on_device(
    positions,
    mass,
    local_tiles,
    local_rows,
    local_cols,
    live_tiles,
    dom_tiles,
    dom_cols,
    dom_slots,
    dom_rows,
    sub_tiles,
    sub_cols,
    sub_slots,
    sub_rows,
    precond,
):
    vector = jax.ShapeDtypeStruct((DIMS, NB, TILE), F32)
    dma = pltpu.SemaphoreType.DMA
    solved, left = pl.pallas_call(
        kernel,
        out_shape=(pltpu.VMEM((DIMS, NB, TILE), F32),) * 2,
        in_specs=[pl.BlockSpec(memory_space=pl.ANY)] * 15,
        out_specs=(pl.BlockSpec(memory_space=pltpu.VMEM),) * 2,
        scratch_shapes=[
            pltpu.VMEM((DIMS, NB * TILE), F32),
            pltpu.VMEM((PHASES, DIMS, NB, TILE), F32),
            pltpu.VMEM((PHASES, NB, 8, TILE), F32),
            pltpu.VMEM((3, DIMS, NB, TILE), F32),
            pltpu.VMEM((3, DIMS, NB, TILE), F32),
            pltpu.VMEM((NB, TILE), F32),
            pltpu.VMEM((2 * PAIRS, TILE, TILE), F32),
            pltpu.VMEM((2 * PAIRS, 2 * TILE + 16, TILE), BF16),
            pltpu.VMEM((ROWS_X * 8, TILE), F32),
            pltpu.VMEM((PAIRS * 16, TILE), F32),
            pltpu.VMEM((DIMS, NB, TILE), F32),
            pltpu.VMEM((PHASES, BITS, DIMS, NB, TILE), F32),
            pltpu.VMEM((PHASES, N_SUB - 1, DIMS, SS, TILE), F32),
            pltpu.VMEM((PHASES, N_SUB - 1, DIMS, SS, TILE), F32),
            pltpu.VMEM((NB, LT), BF16),
            pltpu.VMEM((NB, IFS + IFD), BF16),
            pltpu.VMEM((NEAR_TILES, 2 * DIMS * TILE), BF16),
            pltpu.VMEM((1, LT), jnp.int32),
            pltpu.VMEM((1, IFS), jnp.int32),
            pltpu.VMEM((1, IFD), jnp.int32),
            pltpu.VMEM((1, IFS), jnp.int32),
            pltpu.VMEM((8, TILE), jnp.int32),
            pltpu.VMEM((4, TILE), jnp.int32),
            pltpu.VMEM((BITS, 4, TILE), jnp.int32),
            pltpu.VMEM((24, TILE), F32),
            pltpu.VMEM((8, TILE), F32),
            pltpu.VMEM((4, DIMS, NB, TILE), F32),
            pltpu.VMEM((2, 1, TILE), F32),
            pltpu.VMEM((2, N_DOM * N_SUB, TILE), F32),
            pltpu.SMEM((LT,), jnp.int32),
            pltpu.SMEM((1,), jnp.int32),
            pltpu.SMEM((N_SUB * SS,), jnp.int32),
            pltpu.SMEM((IFD,), jnp.int32),
            pltpu.SMEM((BITS, 4, TILE), jnp.int32),
            pltpu.SMEM((1, IFD), jnp.int32),
            pltpu.SMEM((8, TILE), jnp.int32),
            pltpu.SMEM((2 * PAIR_P,), jnp.int32),
            pltpu.SMEM((3, IFD), jnp.int32),
            dma((12,)),
            dma((2 * PAIRS // GROUP,)),
            dma((BITS,)),
            dma((BITS,)),
            dma,
            dma,
            dma((PHASES, BITS)),
            dma((PHASES, BITS)),
            dma((PHASES, N_SUB - 1)),
            dma((PHASES, N_SUB - 1)),
            dma((2,)),
            dma((2,)),
        ],
        compiler_params=pltpu.CompilerParams(
            collective_id=0, has_side_effects=True, vmem_limit_bytes=56 * 1024 * 1024
        ),
    )(
        positions,
        mass.reshape(NB, TILE),
        local_tiles,
        local_rows,
        local_cols.reshape(1, LT),
        live_tiles,
        dom_tiles,
        dom_cols.reshape(1, IFD),
        dom_slots,
        dom_rows.reshape(4, TILE),
        sub_tiles,
        sub_cols.reshape(1, IFS),
        sub_slots.reshape(1, IFS),
        sub_rows,
        precond,
    )
    return solved.reshape(DIMS, NB * TILE), left.reshape(DIMS, NB * TILE)


def solution(mesh):
    flat = P(("dom", "sub"))
    cube = P(("dom", "sub"), None, None)
    vector = P(None, ("dom", "sub"))
    return jax.shard_map(
        on_device,
        mesh=mesh,
        in_specs=(
            vector,
            flat,
            cube,
            flat,
            flat,
            flat,
            cube,
            flat,
            flat,
            flat,
            cube,
            flat,
            flat,
            flat,
            cube,
        ),
        out_specs=(vector, vector),
        check_vma=False,
    )
```

```python
import functools

import jax
import jax.numpy as jnp
from jax import lax
from jax.experimental import pallas as pl
from jax.experimental.pallas import tpu as pltpu
from jax.sharding import PartitionSpec as P

TILE = 128
DIMS = 3
NB = 32
LT = 64
IFD = 32
IFS = 48
SD = 32
SS = 8
N_DOM = 16
N_SUB = 8
BITS = 4
PHASES = 4
SHIFT = 0.9

PAIR_L = 0
PAIR_S = LT // 2
PAIR_D = PAIR_S + IFS // 2
PAIR_P = PAIR_D + IFD // 2
PAIRS = PAIR_P + NB // 2
GROUP = 16
EARLY = LT // GROUP

FAR = (4, 5, 6, 7)
NEAR = (2, 3, 1)
NEAR_TILES = IFS - len(FAR) * SS

BASE_D = NB
BASE_S = NB + BITS * NB
ROWS_X = BASE_S + N_SUB * SS

F32 = jnp.float32
BF16 = jnp.bfloat16


def kernel(
    pos_h,
    mass_h,
    lt_h,
    lrow_h,
    lcol_h,
    live_h,
    dt_h,
    dcol_h,
    dslot_h,
    drow_h,
    st_h,
    scol_h,
    sslot_h,
    srow_h,
    pt_h,
    sol_o,
    res_o,
    pos_v,
    x_v,
    x3,
    q_v,
    w_v,
    mass_v,
    land,
    tb,
    xg,
    prod,
    acc,
    got_d,
    got_s,
    pack,
    sel_l,
    sel_r,
    held,
    lcol_v,
    scol_v,
    dcol_v,
    sslot_v,
    tab_v,
    drow_v,
    drow_r,
    part,
    bent,
    last_v,
    row,
    rows,
    lrow_m,
    live_m,
    srow_m,
    dslot_m,
    drow_m,
    dcol_m,
    tab_m,
    idx,
    spot,
    in_sem,
    tile_sem,
    ix_send,
    ix_recv,
    ix_loc,
    tab_sem,
    sd_send,
    sd_recv,
    ss_send,
    ss_recv,
    row_send,
    row_recv,
):
    a = lax.axis_index("dom")
    b = lax.axis_index("sub")

    def dom_dev(j):
        return {"dom": jnp.bitwise_xor(a, 1 << j)}

    def sub_dev(m):
        return {"sub": jnp.bitwise_xor(b, m)}

    small = [
        (pos_h, pos_v),
        (drow_h, drow_v),
        (mass_h, mass_v),
        (lrow_h, lrow_m),
        (live_h, live_m),
        (sslot_h, sslot_v),
        (srow_h, srow_m),
        (dslot_h, dslot_m),
        (lcol_h, lcol_v),
        (scol_h, scol_v),
        (dcol_h, dcol_v),
        (dcol_h, dcol_m),
    ]
    small = [
        pltpu.make_async_copy(src, dst, in_sem.at[i]) for i, (src, dst) in enumerate(small)
    ]
    for copy in small:
        copy.start()
    loads = []
    for src, first in ((lt_h, PAIR_L), (st_h, PAIR_S), (dt_h, PAIR_D), (pt_h, PAIR_P)):
        for start in range(0, src.shape[0], GROUP):
            loads.append(
                pltpu.make_async_copy(
                    src.at[pl.ds(start, GROUP)],
                    land.at[pl.ds(2 * first + start, GROUP)],
                    tile_sem.at[len(loads)],
                )
            )
    barrier = pltpu.get_barrier_semaphore()
    for m in (1, 2, 3, 4, 8, 12):
        pl.semaphore_signal(barrier, inc=1, device_id={"dom": jnp.bitwise_xor(a, m)})
    for o in range(1, N_SUB):
        pl.semaphore_signal(barrier, inc=1, device_id=sub_dev(o))

    for copy in loads[:EARLY]:
        copy.start()

    def dom_copy(p, j):
        return pltpu.make_async_remote_copy(
            src_ref=x_v.at[p],
            dst_ref=got_d.at[p, j],
            send_sem=sd_send.at[p, j],
            recv_sem=sd_recv.at[p, j],
            device_id=dom_dev(j),
        )

    def sub_copy(p, m):
        return pltpu.make_async_remote_copy(
            src_ref=pack.at[p, m - 1],
            dst_ref=got_s.at[p, m - 1],
            send_sem=ss_send.at[p, m - 1],
            recv_sem=ss_recv.at[p, m - 1],
            device_id=sub_dev(m),
        )

    def row_copy(j):
        return pltpu.make_async_remote_copy(
            src_ref=drow_v,
            dst_ref=drow_r.at[j],
            send_sem=ix_send.at[j],
            recv_sem=ix_recv.at[j],
            device_id=dom_dev(j),
        )

    def send(p):
        for j in (1, 3):
            dom_copy(p, j).start()

        if isinstance(p, int) and p == 0:
            for copy in small[2:]:
                copy.wait()
        order = FAR + NEAR
        for n, o in enumerate(order):
            for s in range(SS):
                block = srow_m[jnp.bitwise_xor(b, o) * SS + s]
                values = x3[p, block]
                for k in range(DIMS):
                    pack[p, o - 1, k, pl.ds(s, 1), :] = values[k : k + 1]
            if n:
                sub_copy(p, order[n - 1]).start()
        sub_copy(p, order[-1]).start()
        for j in (0, 2):
            dom_copy(p, j).start()

    xg3 = xg.reshape(ROWS_X, 8, TILE)

    def split(base, count, values):
        for k in range(DIMS):
            high = values[k].astype(BF16).astype(F32)
            xg[pl.ds(base * 8 + k, count, stride=8), :] = high
            xg[pl.ds(base * 8 + DIMS + k, count, stride=8), :] = values[k] - high

    def multiply(slot, one, two, first, second):
        left = jnp.concatenate([xg3[first], xg3[second]], axis=0).astype(BF16)
        out = jnp.dot(
            jnp.concatenate([left, left], axis=1),
            jnp.concatenate(
                [tb[one, 0 : 2 * TILE, :], tb[two, 0 : 2 * TILE, :]], axis=1
            ),
            preferred_element_type=F32,
        )
        prod[slot * 16 : slot * 16 + 8, :] = out[0:8, 0:TILE]
        prod[slot * 16 + 8 : slot * 16 + 16, :] = out[8:16, TILE : 2 * TILE]

    def run(first, count):
        for slot in range(first, first + count):
            one = 2 * slot
            multiply(slot, one, one + 1, idx[one], idx[one + 1])

    def run_sub(first, last):
        for t in range(first, last, 2):
            multiply(
                PAIR_S + t // 2,
                2 * PAIR_S + tab_m[0, t],
                2 * PAIR_S + tab_m[0, t + 1],
                tab_m[1, t],
                tab_m[1, t + 1],
            )

    def taken(first, count, k):
        return (
            prod[pl.ds(first * 8 + k, count, stride=8), :]
            + prod[pl.ds(first * 8 + DIMS + k, count, stride=8), :]
        )

    def terms_of(first, count):
        terms = []
        for k in range(DIMS):
            value = taken(first, count, k)
            high = value.astype(BF16)
            terms += [high, (value - high.astype(F32)).astype(BF16)]
        return jnp.concatenate(terms, axis=1)

    def combine(select, terms):
        out = jnp.dot(select[...], terms, preferred_element_type=F32)
        sums = []
        for k in range(DIMS):
            at = 2 * k * TILE
            sums.append(out[:, at + TILE : at + 2 * TILE] + out[:, at : at + TILE])
        return sums

    small[1].wait()
    pl.semaphore_wait(barrier, 6 + N_SUB - 1)
    for j in range(BITS):
        row_copy(j).start()
    small[0].wait()
    for c in range(NB):
        x3[0, c, 0:DIMS, :] = pos_v[:, c * TILE : (c + 1) * TILE]
    for k in range(DIMS):
        x_v[0, k] = x3[0, :, k, :]
    send(0)
    for copy in loads[EARLY:]:
        copy.start()

    block_ids = lax.broadcasted_iota(jnp.int32, (NB, LT), 0)
    tile_ids = lax.broadcasted_iota(jnp.int32, (NB, LT), 1)
    hit = jnp.logical_and(lcol_v[...] == block_ids, tile_ids < live_m[0])
    sel_l[...] = jnp.where(hit, 1.0, 0.0).astype(BF16)
    square = (IFS, IFS)
    down = lax.broadcasted_iota(jnp.int32, square, 0)
    across = lax.broadcasted_iota(jnp.int32, square, 1)

    def stand(values):
        return jnp.sum(
            jnp.where(down == across, values.astype(F32), 0.0), axis=1, keepdims=True
        )

    slot = sslot_v[...]
    apart = jnp.bitwise_xor(jnp.right_shift(slot, 3), b)
    place = BASE_S + (apart - 1) * SS + jnp.bitwise_and(slot, SS - 1)
    key = lax.broadcasted_iota(jnp.int32, (1, IFS), 1) + jnp.where(
        apart >= 4, TILE, 0
    )
    keys = stand(key)
    rank = jnp.sum(
        jnp.where(key.astype(F32) < keys, 1.0, 0.0), axis=1, keepdims=True
    )
    chosen = jnp.where(rank == across.astype(F32), 1.0, 0.0)
    tab_v[...] = jnp.zeros_like(tab_v)
    ranges = (IFS, ROWS_X, NB)
    for n, values in enumerate((down.astype(F32), stand(place), stand(scol_v[...]))):
        line = jnp.sum(chosen * values, axis=0, keepdims=True).astype(jnp.int32)
        line = jnp.clip(line, 0, ranges[n] - 1)
        tab_v[n : n + 1, 0:IFS] = line
    tabled = pltpu.make_async_copy(tab_v, tab_m, tab_sem)
    tabled.start()
    sel_r[:, 0:IFS] = jnp.where(
        line == lax.broadcasted_iota(jnp.int32, (NB, IFS), 0), 1.0, 0.0
    ).astype(BF16)
    sel_r[:, IFS : IFS + IFD] = jnp.where(
        dcol_v[...] == lax.broadcasted_iota(jnp.int32, (NB, IFD), 0), 1.0, 0.0
    ).astype(BF16)
    xg[...] = jnp.zeros_like(xg)

    def put_local(t, carry):
        idx[t] = lrow_m[t]
        return carry

    lax.fori_loop(0, LT, put_local, 0, unroll=8)

    def convert(i):
        for half in range(2):
            tile = land[2 * i + half]
            high = tile.astype(BF16)
            low = (tile - high.astype(F32)).astype(BF16)
            tb[2 * i + half, 0:TILE, :] = high
            tb[2 * i + half, TILE : 2 * TILE, :] = low

    def arrive(first, count):
        def body(n, carry):
            pltpu.make_async_copy(
                lt_h.at[pl.ds(0, GROUP)],
                land.at[pl.ds(n * GROUP, GROUP)],
                tile_sem.at[n],
            ).wait()
            for i in range(GROUP // 2):
                convert(n * GROUP // 2 + i)
            return carry

        lax.fori_loop(first * 2 // GROUP, (first + count) * 2 // GROUP, body, 0)

    def put_place(t, carry):
        slot = dslot_m[t]
        other = jnp.bitwise_xor(jnp.right_shift(slot, 5), a)
        bit = (
            (other >= 2).astype(jnp.int32)
            + (other >= 4).astype(jnp.int32)
            + (other >= 8).astype(jnp.int32)
        )
        place = a * SD + jnp.bitwise_and(slot, SD - 1)
        spot[0, t] = bit
        spot[1, t] = jnp.right_shift(place, 7)
        spot[2, t] = jnp.bitwise_and(place, TILE - 1)
        return carry

    lax.fori_loop(0, IFD, put_place, 0, unroll=8)

    def put_dom(t, carry):
        bit = spot[0, t]
        block = drow_m[bit, spot[1, t], spot[2, t]]
        idx[2 * PAIR_D + t] = BASE_D + bit * NB + block
        return carry

    part[...] = jnp.zeros_like(part)
    wanted = [(0, 0), (0, 1), (0, 2), (1, 1), (1, 2), (2, 2)]
    moved = pltpu.make_async_copy(drow_r, drow_m, ix_loc)
    me = a * N_SUB + b
    count = N_DOM * N_SUB

    def hops(m):
        return sum((0, 1, 2, 1)[(m >> at) & 3] for at in (1, 3, 5))

    def row_to(which, m):
        other = jnp.bitwise_xor(me, m)
        return pltpu.make_async_remote_copy(
            src_ref=row.at[which],
            dst_ref=rows.at[which, pl.ds(me, 1)],
            send_sem=row_send.at[which],
            recv_sem=row_recv.at[which],
            device_id={
                "dom": jnp.right_shift(other, 3),
                "sub": jnp.bitwise_and(other, N_SUB - 1),
            },
        )

    def row_all(which):
        everyone = rows.at[which, pl.ds(0, count - 1)]
        return pltpu.make_async_remote_copy(
            src_ref=everyone,
            dst_ref=everyone,
            send_sem=row_send.at[which],
            recv_sem=row_recv.at[which],
            device_id=sub_dev(1),
        )

    def to_row(which, table):
        sums = jnp.sum(table, axis=1, keepdims=True)
        eye = lax.broadcasted_iota(jnp.int32, table.shape, 0) == lax.broadcasted_iota(
            jnp.int32, table.shape, 1
        )
        value = jnp.sum(jnp.where(eye, sums, 0.0), axis=0, keepdims=True)
        row[which] = value
        rows[which, pl.ds(me, 1), :] = value

    def early_rows():
        for n, (i, j) in enumerate(wanted):
            for k in range(DIMS):
                part[pl.ds(n * DIMS + k, 1), :] = jnp.sum(
                    q_v[i, k] * x_v[j + 1, k], axis=0, keepdims=True
                )
        to_row(0, part[...])

        def body(i, carry):
            row_to(0, i + 1).start()
            return carry

        lax.fori_loop(0, count - 1, body, 0, unroll=4)

    def met(p, first, count, table, line, start=0):
        total = None
        for t in range(count):
            at = (first + t) * 8
            term = x3[p, table[line, start + t]] * prod[at : at + 8, :]
            total = term if total is None else total + term
        return total

    def drain(p):
        for j in range(BITS):
            dom_copy(p, j).wait_send()
        for m in range(1, N_SUB):
            sub_copy(p, m).wait_send()

    def phase(p, first, last):
        if first:
            arrive(PAIR_L, LT // 2)
        else:
            send(p)
        split(0, NB, [x_v[p, k] for k in range(DIMS)])
        run(PAIR_L, LT // 2)
        if first:
            for j in range(BITS):
                row_copy(j).wait_recv()
            moved.start()
            arrive(PAIR_S, IFS // 2)
        if first:
            for j in range(BITS):
                row_copy(j).wait_send()
        else:
            drain(p - 1)
        inner = combine(sel_l, terms_of(2 * PAIR_L, LT))
        for k in range(DIMS):
            acc[k] = mass_v[...] * x_v[p, k] + inner[k]
        if last:
            early_rows()
            for k in range(DIMS):
                x3[p, :, DIMS + k, :] = x_v[p, k]
        def take(ms):
            for m in ms:
                sub_copy(p, m).wait_recv()
                split(
                    BASE_S + (m - 1) * SS, SS, [got_s[p, m - 1, k] for k in range(DIMS)]
                )

        if first:
            tabled.wait()
        take(NEAR[::-1])
        run_sub(0, NEAR_TILES)
        held[...] = terms_of(2 * PAIR_S, NEAR_TILES)
        if last:
            bent[...] = met(p, 2 * PAIR_S, NEAR_TILES, tab_m, 2)
            for k in range(DIMS):
                bent[k : k + 1, :] += jnp.sum(
                    acc[k] * x_v[p, k], axis=0, keepdims=True
                )
        if first:
            arrive(PAIR_D, IFD // 2)
            arrive(PAIR_P, NB // 2)
        take(FAR)
        run_sub(NEAR_TILES, IFS)
        if first:
            moved.wait()
            lax.fori_loop(0, IFD, put_dom, 0, unroll=True)
        for j in (1, 3, 0, 2):
            dom_copy(p, j).wait_recv()
            split(BASE_D + j * NB, NB, [got_d[p, j, k] for k in range(DIMS)])
        run(PAIR_D, IFD // 2)
        if last:
            whole = bent[...] + met(
                p, 2 * PAIR_S + NEAR_TILES, IFS - NEAR_TILES, tab_m, 2, NEAR_TILES
            )
            whole = whole + met(p, 2 * PAIR_D, IFD, dcol_m, 0)
            to_row(1, whole[0:DIMS] + whole[DIMS : 2 * DIMS])
            for m in sorted(range(1, count), key=lambda m: -hops(m)):
                row_to(1, m).start()
        outer = combine(
            sel_r,
            jnp.concatenate(
                [
                    held[...],
                    terms_of(2 * PAIR_S + NEAR_TILES, IFS - NEAR_TILES + IFD),
                ],
                axis=0,
            ),

        )
        for k in range(DIMS):
            value = acc[k] + outer[k]
            if first:
                q_v[0, k] = mass_v[...] * x_v[0, k] - value
            else:
                w_v[p - 1, k] = value
                if not last:
                    q_v[p, k] = value - SHIFT * q_v[p - 1, k]
        if not last:
            split(0, NB, [q_v[p, k] for k in range(DIMS)])
            for i in range(NB // 2):
                one = 2 * (PAIR_P + i)
                multiply(PAIR_P + i, one, one + 1, 2 * i, 2 * i + 1)
            for k in range(DIMS):
                value = taken(2 * PAIR_P, NB, k)
                x_v[p + 1, k] = value
                x3[p + 1, :, k, :] = value

    def later(p, carry):
        phase(p, False, False)
        return carry

    phase(0, True, False)
    lax.fori_loop(1, PHASES - 1, later, 0)
    phase(PHASES - 1, False, True)

    drain(PHASES - 1)
    row_all(0).wait_send()
    row_all(0).wait_recv()
    wide = jnp.broadcast_to(jnp.sum(rows[0], axis=0, keepdims=True), (8, TILE))
    values = [wide] + [pltpu.roll(wide, TILE - DIMS * n, 1) for n in range(1, 6)]
    gram = {}
    for (i, j), value in zip(wanted, values):
        gram[i, j] = gram[j, i] = value
    curve = {}
    for j in range(2):
        for i in range(3):
            curve[i, j] = curve[j, i] = gram[i, j + 1] + SHIFT * gram[i, j]

    def form(table, vector):
        out = None
        for i in range(len(vector)):
            for j in range(i, len(vector)):
                if (i, j) in table:
                    term = vector[i] * vector[j] * table[i, j]
                    term = term if i == j else 2.0 * term
                    out = term if out is None else out + term
        return out

    one = jnp.ones((8, TILE), F32)
    rho = [one]
    along = [one]
    current = gram[0, 0]
    solved = []
    for it in range(2):
        step = current / form(curve, along)
        for i, value in enumerate(along):
            if i < len(solved):
                solved[i] = solved[i] + step * value
            else:
                solved.append(step * value)
        fresh = []
        for i in range(len(along) + 1):
            value = rho[i] if i < len(rho) else None
            if i < len(along):
                value = value - step * (SHIFT * along[i])
            if i > 0:
                less = step * along[i - 1]
                value = -less if value is None else value - less
            fresh.append(value)
        rho = fresh
        following = form(gram, rho)
        ratio = following / current
        along = [
            value + ratio * along[i] if i < len(along) else value
            for i, value in enumerate(rho)
        ]
        current = following
    known = form(curve, along)
    square = along[2] * along[2]
    for k in range(DIMS):
        faired, left = x_v[0, k], q_v[0, k]
        turn, lift = None, None
        for j in range(3):
            scale = along[j][0:1, k : k + 1]
            turn = scale * x_v[j + 1, k] if j == 0 else turn + scale * x_v[j + 1, k]
            lift = scale * w_v[j, k] if j == 0 else lift + scale * w_v[j, k]
            if j < 2:
                scale = solved[j][0:1, k : k + 1]
                faired = faired + scale * x_v[j + 1, k]
                left = left - scale * w_v[j, k]
        last_v[0, k] = faired
        last_v[1, k] = turn
        last_v[2, k] = left
        last_v[3, k] = lift
    row_all(1).wait_recv()
    step = current / (known + square * jnp.sum(rows[1], axis=0, keepdims=True))
    for k in range(DIMS):
        scale = step[0:1, k : k + 1]
        sol_o[k] = last_v[0, k] + scale * last_v[1, k]
        res_o[k] = last_v[2, k] - scale * last_v[3, k]

    row_all(1).wait_send()


def on_device(
    positions,
    mass,
    local_tiles,
    local_rows,
    local_cols,
    live_tiles,
    dom_tiles,
    dom_cols,
    dom_slots,
    dom_rows,
    sub_tiles,
    sub_cols,
    sub_slots,
    sub_rows,
    precond,
):
    vector = jax.ShapeDtypeStruct((DIMS, NB, TILE), F32)
    dma = pltpu.SemaphoreType.DMA
    solved, left = pl.pallas_call(
        kernel,
        out_shape=(pltpu.VMEM((DIMS, NB, TILE), F32),) * 2,
        in_specs=[pl.BlockSpec(memory_space=pl.ANY)] * 15,
        out_specs=(pl.BlockSpec(memory_space=pltpu.VMEM),) * 2,
        scratch_shapes=[
            pltpu.VMEM((DIMS, NB * TILE), F32),
            pltpu.VMEM((PHASES, DIMS, NB, TILE), F32),
            pltpu.VMEM((PHASES + 1, NB, 8, TILE), F32),
            pltpu.VMEM((3, DIMS, NB, TILE), F32),
            pltpu.VMEM((3, DIMS, NB, TILE), F32),
            pltpu.VMEM((NB, TILE), F32),
            pltpu.VMEM((2 * PAIRS, TILE, TILE), F32),
            pltpu.VMEM((2 * PAIRS, 2 * TILE + 16, TILE), BF16),
            pltpu.VMEM((ROWS_X * 8, TILE), F32),
            pltpu.VMEM((PAIRS * 16 + 8, TILE), F32),
            pltpu.VMEM((DIMS, NB, TILE), F32),
            pltpu.VMEM((PHASES, BITS, DIMS, NB, TILE), F32),
            pltpu.VMEM((PHASES, N_SUB - 1, DIMS, SS, TILE), F32),
            pltpu.VMEM((PHASES, N_SUB - 1, DIMS, SS, TILE), F32),
            pltpu.VMEM((NB, LT), BF16),
            pltpu.VMEM((NB, IFS + IFD), BF16),
            pltpu.VMEM((NEAR_TILES, 2 * DIMS * TILE), BF16),
            pltpu.VMEM((1, LT), jnp.int32),
            pltpu.VMEM((1, IFS), jnp.int32),
            pltpu.VMEM((1, IFD), jnp.int32),
            pltpu.VMEM((1, IFS), jnp.int32),
            pltpu.VMEM((8, TILE), jnp.int32),
            pltpu.VMEM((4, TILE), jnp.int32),
            pltpu.VMEM((BITS, 4, TILE), jnp.int32),
            pltpu.VMEM((24, TILE), F32),
            pltpu.VMEM((8, TILE), F32),
            pltpu.VMEM((4, DIMS, NB, TILE), F32),
            pltpu.VMEM((2, 1, TILE), F32),
            pltpu.VMEM((2, N_DOM * N_SUB, TILE), F32),
            pltpu.SMEM((LT,), jnp.int32),
            pltpu.SMEM((1,), jnp.int32),
            pltpu.SMEM((N_SUB * SS,), jnp.int32),
            pltpu.SMEM((IFD,), jnp.int32),
            pltpu.SMEM((BITS, 4, TILE), jnp.int32),
            pltpu.SMEM((1, IFD), jnp.int32),
            pltpu.SMEM((8, TILE), jnp.int32),
            pltpu.SMEM((2 * PAIR_P,), jnp.int32),
            pltpu.SMEM((3, IFD), jnp.int32),
            dma((12,)),
            dma((2 * PAIRS // GROUP,)),
            dma((BITS,)),
            dma((BITS,)),
            dma,
            dma,
            dma((PHASES, BITS)),
            dma((PHASES, BITS)),
            dma((PHASES, N_SUB - 1)),
            dma((PHASES, N_SUB - 1)),
            dma((2,)),
            dma((2,)),
        ],
        compiler_params=pltpu.CompilerParams(
            collective_id=0, has_side_effects=True, vmem_limit_bytes=56 * 1024 * 1024
        ),
    )(
        positions,
        mass.reshape(NB, TILE),
        local_tiles,
        local_rows,
        local_cols.reshape(1, LT),
        live_tiles,
        dom_tiles,
        dom_cols.reshape(1, IFD),
        dom_slots,
        dom_rows.reshape(4, TILE),
        sub_tiles,
        sub_cols.reshape(1, IFS),
        sub_slots.reshape(1, IFS),
        sub_rows,
        precond,
    )
    return solved.reshape(DIMS, NB * TILE), left.reshape(DIMS, NB * TILE)


def solution(mesh):
    flat = P(("dom", "sub"))
    cube = P(("dom", "sub"), None, None)
    vector = P(None, ("dom", "sub"))
    return jax.shard_map(
        on_device,
        mesh=mesh,
        in_specs=(
            vector,
            flat,
            cube,
            flat,
            flat,
            flat,
            cube,
            flat,
            flat,
            flat,
            cube,
            flat,
            flat,
            flat,
            cube,
        ),
        out_specs=(vector, vector),
        check_vma=False,
    )
```
